32 devices in a mesh: dp: 32 (over z, y, x, core).
Axes of the slice: x: 2, y: 2, z: 4, core: 2. Of those that a mesh axis runs over, the one named last changes fastest.
Arguments:
- query_features: bfloat16 [8192, 768], P('dp'), may hold values from -24 to 24
- passage_features: bfloat16 [8192, 768], P('dp'), may hold values from -24 to 24
- counts: int32 [32], replicated, may hold values from 128 to 256, as said below
- positives: int32 [8192], P('dp'), may hold values from 0 to 4351
- w_first: bfloat16 [768, 1536], replicated, may hold values from -0.21875 to 0.21875
- w_second: bfloat16 [1536, 384], replicated, may hold values from -0.15625 to 0.15625
Outputs:
- mean_loss: float32 [], replicated
- grad_first: float32 [768, 1536], P(None, 'dp')
- grad_second: float32 [1536, 384], P('dp')
The draws below stay inside these ranges and needn't reach their ends.
Inputs may be any that keep to these rules, and one draw needn't show every extreme that they name: Device i holds counts[i] pairs in the first slots of its 256 slots. Each entry is 128 or 256; among the 16 devices whose indices agree modulo 32 // 16 exactly one entry is 256, so the entries sum to 4352. `positives`: only entries of occupied slots are used; an entry is the index of a passage in the order of occupied slots, device by device.
All inputs are finite; a program needn't handle non-finite values.
Results may differ from the reference program's by a relative error of at most 0.0043.
The reference program's roundings to bfloat16 on the way count: a program that leaves them out, or rounds other values in their place, can miss the bound.
Values may be sent and summed in bfloat16 or wider, within the bound.
A program may use at most 128 MiB of HBM per device.

```python
import jax
import jax.numpy as jnp
from jax import lax

D = 768
FF = 1536
E = 384
LOW = 128
BLOCK = 136
CAP = 256
PAIRS = 4352
N_DP = 32


def feature_pair(key):
    pass_key = jax.random.fold_in(key, 11)
    query_key = jax.random.fold_in(key, 12)
    shape = (N_DP * CAP, D)
    passages = jax.random.truncated_normal(pass_key, -4.0, 4.0, shape, jnp.float32)
    queries = jax.random.truncated_normal(query_key, -4.0, 4.0, shape, jnp.float32)
    return (queries, passages)


def draw_query_features(key, part):
    return feature_pair(key)[0].astype(jnp.bfloat16)


def draw_passage_features(key, part):
    return feature_pair(key)[1].astype(jnp.bfloat16)


def draw_counts(key, part):
    stride = N_DP // 16
    heavy_pos = jax.random.randint(key, (stride,), 0, 16)
    device_ids = jnp.arange(N_DP, dtype=jnp.int32)
    heavy = device_ids // stride == heavy_pos[device_ids % stride]
    return (LOW + LOW * heavy.astype(jnp.int32)).astype(jnp.int32)


def place_ends(values, rng, smallest, high):
    shape = values.shape
    index_at = [jax.random.randint(jax.random.fold_in(rng, axis), (), 0, shape[axis]) for axis in range(len(shape))]
    values = values.at[tuple(index_at)].set(smallest)
    longest = shape.index(max(shape))
    index_at[longest] = (index_at[longest] + 1) % shape[longest]
    return values.at[tuple(index_at)].set(high)


def normal_values(key, shape, spread, most, held_as=jnp.bfloat16):
    result = spread * jax.random.normal(key, shape, jnp.float32)
    return jnp.clip(result, min=-most, max=most).astype(held_as)


def setup_inputs(seed: int = 0) -> dict:
    keys = jax.random.split(jax.random.key(seed), 7)
    return {
        "query_features": draw_query_features(jax.random.fold_in(keys[6], 71), 0),
        "passage_features": draw_passage_features(jax.random.fold_in(keys[6], 71), 0),
        "counts": draw_counts(jax.random.fold_in(keys[6], 71), 0),
        "positives": place_ends(jax.random.randint(keys[3], (N_DP * CAP,), 0, PAIRS), jax.random.fold_in(keys[3], 1), 0, PAIRS - 1).astype(jnp.int32),
        "w_first": normal_values(keys[4], (D, FF), D ** -0.5, 0.21875),
        "w_second": normal_values(keys[5], (FF, E), FF ** -0.5, 0.15625),
    }


def gelu_tanh(values):
    return jax.nn.gelu(values, approximate=True)

def tower_pass(features, w_first, w_second):
    pre_act = jnp.dot(features, w_first, preferred_element_type=jnp.float32)
    hidden = gelu_tanh(pre_act).astype(jnp.bfloat16)
    embedded = jnp.dot(hidden, w_second, preferred_element_type=jnp.float32).astype(jnp.bfloat16)
    return (pre_act, hidden, embedded)

def weight_terms(features, pre_act, hidden, grads, w_second):
    grad_second = lax.dot_general(hidden, grads, (((0,), (0,)), ((), ())), preferred_element_type=jnp.float32)
    back_act = lax.dot_general(grads, w_second, (((1,), (1,)), ((), ())), preferred_element_type=jnp.float32)
    pull_back = jax.vjp(gelu_tanh, pre_act)[1]
    pre_grad = pull_back(back_act)[0].astype(jnp.bfloat16)
    grad_first = lax.dot_general(features, pre_grad, (((0,), (0,)), ((), ())), preferred_element_type=jnp.float32)
    return (grad_first, grad_second)

def reference(query_features, passage_features, counts, positives, w_first, w_second):
    slot_ids = jnp.arange(N_DP * CAP, dtype=jnp.int32)
    owner_dev = slot_ids // CAP
    row_in = slot_ids % CAP
    offsets = (jnp.cumsum(counts) - counts).astype(jnp.int32)
    occupied = row_in < counts[owner_dev]
    dest_row = jnp.where(occupied, offsets[owner_dev] + row_in, PAIRS).astype(jnp.int32)
    width = query_features.shape[1]
    queries_in = jnp.zeros((PAIRS, width), query_features.dtype).at[dest_row].set(query_features, mode='drop')
    passages_in = jnp.zeros((PAIRS, width), passage_features.dtype).at[dest_row].set(passage_features, mode='drop')
    positive_ids = jnp.zeros((PAIRS,), jnp.int32).at[dest_row].set(positives, mode='drop')
    pre_q, hidden_q, query_emb = tower_pass(queries_in, w_first, w_second)
    pre_p, hidden_p, passage_emb = tower_pass(passages_in, w_first, w_second)
    score_scale = 2.5 * E ** (-0.5)
    step_rows = BLOCK * 16
    step_count = PAIRS // step_rows
    columns = jnp.arange(PAIRS, dtype=jnp.int32)

    def one_step(grad_sum, step_index):
        query_rows = lax.dynamic_slice_in_dim(query_emb, step_index * step_rows, step_rows, 0)
        pos_rows = lax.dynamic_slice_in_dim(positive_ids, step_index * step_rows, step_rows, 0)
        scores = lax.dot_general(query_rows, passage_emb, (((1,), (1,)), ((), ())), preferred_element_type=jnp.float32) * score_scale
        row_top = lax.optimization_barrier(jnp.max(scores, axis=1))
        log_norm = row_top + jnp.log(lax.optimization_barrier(jnp.sum(jnp.exp(scores - row_top[:, None]), axis=1)))
        is_positive = pos_rows[:, None] == columns[None, :]
        pos_score = lax.optimization_barrier(jnp.sum(jnp.where(is_positive, scores, jnp.zeros_like(scores)), axis=1))
        weights = (jnp.exp(scores - log_norm[:, None]) - is_positive.astype(jnp.float32)).astype(jnp.bfloat16)
        query_grad = (score_scale * jnp.dot(weights, passage_emb, preferred_element_type=jnp.float32)).astype(jnp.bfloat16)
        grad_sum = grad_sum + lax.dot_general(weights, query_rows, (((0,), (0,)), ((), ())), preferred_element_type=jnp.float32)
        return (grad_sum, (query_grad, jnp.sum(log_norm - pos_score)))
    start_sum = jnp.zeros((PAIRS, query_emb.shape[1]), jnp.float32)
    grad_sum, (query_parts, loss_parts) = lax.scan(one_step, start_sum, jnp.arange(step_count, dtype=jnp.int32))
    query_grads = query_parts.reshape(PAIRS, query_emb.shape[1])
    passage_grads = (score_scale * grad_sum).astype(jnp.bfloat16)
    mean_loss = jnp.sum(loss_parts) / PAIRS
    first_q, second_q = weight_terms(queries_in, pre_q, hidden_q, query_grads, w_second)
    first_p, second_p = weight_terms(passages_in, pre_p, hidden_p, passage_grads, w_second)
    return (mean_loss, first_q + first_p, second_q + second_p)
```

```python
import functools

import jax
import jax.numpy as jnp
from jax import lax
from jax.experimental import pallas as pl
from jax.experimental.pallas import tpu as pltpu
from jax.sharding import PartitionSpec as P

MESH = pl.DeviceIdType.MESH
F32 = jnp.float32
BF16 = jnp.bfloat16
GELU_ROOT = 0.7978845608028654
GELU_CUBE = 0.044715
TILES = 2
AHEAD = 3
DELAY = 2


def gelu_and_slope(value):
    square = value * value
    bent = jnp.tanh(GELU_ROOT * value * (1.0 + GELU_CUBE * square))
    rise = 0.5 * (1.0 + bent)
    slope = rise + 0.5 * value * (1.0 - bent * bent) * (
        GELU_ROOT * (1.0 + 3.0 * GELU_CUBE * square)
    )
    return value * rise, slope


def dot(left, right, left_dim, right_dim):
    return lax.dot_general(
        left, right, (((left_dim,), (right_dim,)), ((), ())), preferred_element_type=F32
    )


def flat_rows(blocks):
    return blocks.astype(F32).reshape(-1, blocks.shape[-1]).astype(BF16)


class Group:
    def __init__(self, send, recv):
        self.send, self.recv = send, recv

    def start(self, source, landing, device):
        pltpu.make_async_remote_copy(
            src_ref=source,
            dst_ref=landing,
            send_sem=self.send,
            recv_sem=self.recv,
            device_id=(device,),
            device_id_type=MESH,
        ).start()

    def landed(self, span):
        pltpu.make_async_copy(span, span, self.recv).wait()

    def sent(self, span):
        pltpu.make_async_copy(span, span, self.send).wait()

    def done(self, span):
        self.landed(span)
        self.sent(span)


class Groups:
    def __init__(self, send, recv):
        self.send, self.recv, self.used = send, recv, 0

    def new(self):
        self.used += 1
        return Group(self.send.at[self.used - 1], self.recv.at[self.used - 1])


def step_kernel(
    size,
    plane,
    score_scale,
    counts,
    query_hbm,
    passage_hbm,
    positives,
    w_first_hbm,
    w_second_hbm,
    out_loss,
    out_all,
    units,
    unit_mid,
    unit_pass,
    unit_land,
    unit_pos,
    feat_base,
    feat_tail,
    q_base,
    q_tail,
    p_base,
    p_tail,
    pos_land,
    all_q,
    all_p,
    scores,
    stat_land,
    dq_own_base,
    dq_own_tail,
    dq_out_base,
    dq_out_tail,
    dq_land_base,
    dq_land_tail,
    dp_own_base,
    dp_own_tail,
    dp_out_base,
    dp_out_tail,
    dp_land_base,
    dp_land_tail,
    loss_land,
    de_base,
    de_tail,
    own_tail,
    all_x,
    own,
    outgoing,
    landing,
    outgoing_two,
    landing_two,
    sums,
    forward,
    landed,
    send_sems,
    recv_sems,
    line_send,
    line_recv,
    w_first,
    w_second,
    all_hidden,
    all_slope,
    load_sems,
):
    me = lax.axis_index("dp")
    rows = size // plane
    half = rows // 2
    lanes = plane // 2
    stride = size // 16
    row = lax.div(me, plane)
    spot = lax.rem(me, plane)
    core = lax.rem(me, 2)
    lane = lax.div(spot, 2)
    column = spot - core
    place = lax.div(me, stride)
    partner = me + 1 - 2 * core
    width, hidden_width = w_first.shape
    embed = w_second.shape[1]
    base = q_base.shape[1]
    unit = q_tail.shape[1]
    hidden_half = hidden_width // 2
    tile = hidden_half // TILES
    per_tile = half // TILES
    chunk = hidden_half // (half * lanes * 2)
    groups = Groups(send_sems, recv_sems)

    plane_peers = [row * plane + lax.rem(spot + k, plane) for k in range(1, plane)]
    line_peers = [lax.rem(row + k, rows) * plane + spot for k in range(1, rows)]
    barrier = pltpu.get_barrier_semaphore()

    def greet(device):
        pl.semaphore_signal(barrier, inc=1, device_id=(device,), device_id_type=MESH)

    for k in range(1, 16):
        greet(lax.rem(place + k, 16) * stride + lax.rem(me, stride))
    for device in plane_peers:
        greet(device)
    in_column = 2 * row + core
    for k in range(1, 2 * rows):
        other = lax.rem(in_column + k, 2 * rows)
        greet(plane * lax.div(other, 2) + column + lax.rem(other, 2))

    spare = base + unit
    near = plane // stride
    aside = lax.div(spot, stride)
    for at, (features, sem) in enumerate(((query_hbm, 0), (passage_hbm, 1))):
        side = pl.ds(at * width, width)
        for u in range(15):
            there = u + lax.div(u + 16 - place, 16)
            pltpu.make_async_copy(
                features.at[pl.ds(spare + u * unit, unit), :],
                units.at[lax.div(there, near), lax.rem(there, near), :, side],
                load_sems.at[sem],
            ).start()
    base_loads = [
        pltpu.make_async_copy(
            features.at[pl.ds(0, base), :], feat_base.at[core, at], load_sems.at[2 + at]
        )
        for at, features in enumerate((query_hbm, passage_hbm))
    ]
    weight_loads = [
        pltpu.make_async_copy(w_first_hbm, w_first, load_sems.at[4]),
        pltpu.make_async_copy(w_second_hbm, w_second, load_sems.at[5]),
    ]
    tail_loads = [
        pltpu.make_async_copy(
            features.at[pl.ds(base, unit), :], own_tail.at[at], load_sems.at[6 + at]
        )
        for at, features in enumerate((query_hbm, passage_hbm))
    ]
    for load in base_loads + weight_loads + tail_loads:
        load.start()
    unit_pos[place] = positives[...].astype(F32)

    pl.semaphore_wait(barrier, 15 + plane - 1 + 2 * rows - 1)
    for features, sem in ((query_hbm, 0), (passage_hbm, 1)):
        extra = features.at[pl.ds(spare, 15 * unit), :]
        pltpu.make_async_copy(extra, extra, load_sems.at[sem]).wait()

    mid_group = groups.new()
    for k in range(1, near):
        there = lax.rem(aside + k, near)
        mid_group.start(
            units.at[:, there],
            unit_mid.at[aside],
            row * plane + there * stride + lax.rem(me, stride),
        )
    where_group = groups.new()
    for k in range(1, 16):
        device = lax.rem(place + k, 16) * stride + lax.rem(me, stride)
        where_group.start(unit_pos.at[place], unit_pos.at[place], device)

    heavies = []
    for g in range(stride):
        at = jnp.int32(0)
        for k in range(16):
            at = at + jnp.where(counts[g + stride * k] > base, g + stride * k, 0)
        heavies.append(at)
    source = jnp.int32(0)
    for g in range(stride):
        source = source + jnp.where(lax.rem(me, stride) == g, heavies[g], 0)
    heavy_place = jnp.int32(0)
    for k in range(16):
        heavy_place = heavy_place + jnp.where(source >= stride * (k + 1), 1, 0)

    def offset_of(device):
        before = jnp.int32(0)
        for at in heavies:
            before = before + jnp.where(at < device, 1, 0)
        return base * (device + before)

    def tail_row(device):
        piece = lax.div(device, stride) - jnp.where(source < device, 1, 0)
        return jnp.where(source == device, base, spare + unit * piece)

    def tower(features):
        total = None
        for low in range(0, hidden_width, tile):
            act = dot(features, w_first[:, low : low + tile], 1, 0)
            hidden = gelu_and_slope(act)[0].astype(BF16)
            part = dot(hidden, w_second[low : low + tile, :], 1, 0)
            total = part if total is None else total + part
        return total.astype(BF16)

    for load in base_loads:
        load.wait()
    pair_base = groups.new()
    pair_base.start(feat_base.at[core], feat_base.at[core], partner)
    for load in weight_loads:
        load.wait()
    embedded = tower(feat_base[core].reshape(2 * base, width))
    q_base[spot] = embedded[:base]
    p_base[row] = embedded[base:]
    q_group, p_group = groups.new(), groups.new()
    for device in plane_peers:
        q_group.start(q_base.at[spot], q_base.at[spot], device)
    mid_group.done(unit_mid.at[pl.ds(0, near - 1)])
    source_row, source_aside = jnp.int32(0), heavy_place
    for k in range(1, rows):
        beyond = heavy_place >= k * near
        source_row = source_row + jnp.where(beyond, 1, 0)
        source_aside = source_aside - jnp.where(beyond, near, 0)
    unit_pass[...] = jnp.where(source_aside == aside, units[:, aside], unit_mid[source_aside])
    pass_group = groups.new()
    for k in range(1, rows):
        there = lax.rem(row + k, rows)
        pass_group.start(unit_pass.at[there], unit_land.at[row], there * plane + spot)
    for device in line_peers:
        p_group.start(p_base.at[row], p_base.at[row], device)

    where_group.done(unit_pos.at[pl.ds(0, 15)])
    pass_group.done(unit_land.at[pl.ds(0, rows - 1)])
    for load in tail_loads:
        load.wait()
    heavy = source == me
    got = jnp.where(source_row == row, unit_pass[row], unit_land[source_row]).astype(F32)
    tail_q = jnp.where(heavy, own_tail[0].astype(F32), got[:, :width])
    tail_p = jnp.where(heavy, own_tail[1].astype(F32), got[:, width:])
    slots = lax.broadcasted_iota(jnp.int32, (unit, positives.shape[1]), 1)
    chosen = lax.broadcasted_iota(jnp.int32, slots.shape, 0) + tail_row(me)
    tail_pos = jnp.sum(
        jnp.where(slots == chosen, unit_pos[heavy_place], 0.0), axis=1, keepdims=True
    )
    tail_x = jnp.concatenate([tail_q, tail_p], axis=0)
    feat_tail[core] = tail_x.reshape(2, unit, width).astype(BF16)
    tail_e = tower(tail_x.astype(BF16)).astype(F32)
    q_tail[spot] = tail_e[:unit].astype(BF16)
    p_tail[row] = tail_e[unit:].astype(BF16)
    pos_land[spot, 0] = positives[:, :base].astype(F32)
    sub = lax.broadcasted_iota(jnp.int32, (unit, base), 0) + spot * unit
    along = lax.broadcasted_iota(jnp.int32, (unit, base), 1)
    pos_land[spot, 1] = jnp.sum(jnp.where(sub == along, tail_pos, 0.0), axis=0, keepdims=True)
    q_tail_group, p_tail_group, pos_group = groups.new(), groups.new(), groups.new()
    for device in plane_peers:
        pos_group.start(pos_land.at[spot], pos_land.at[spot], device)
        q_tail_group.start(q_tail.at[spot], q_tail.at[spot], device)
    for device in line_peers:
        p_tail_group.start(p_tail.at[row], p_tail.at[row], device)
    pair_tail = groups.new()
    pair_tail.start(feat_tail.at[core], feat_tail.at[core], partner)
    q_group.done(q_base.at[pl.ds(0, plane - 1)])
    q_tail_group.done(q_tail.at[pl.ds(0, plane - 1)])
    pos_group.done(pos_land.at[pl.ds(0, plane - 1)])
    p_group.done(p_base.at[pl.ds(0, rows - 1)])
    p_tail_group.done(p_tail.at[pl.ds(0, rows - 1)])

    q_rows, p_rows = plane * base, rows * base
    all_q[:q_rows] = q_base[...].reshape(q_rows, embed)
    all_q[q_rows:] = flat_rows(q_tail[...])
    all_p[:p_rows] = p_base[...].reshape(p_rows, embed)
    all_p[p_rows:] = flat_rows(p_tail[...])
    pos_tail = pos_land[0, 1]
    for k in range(1, plane):
        pos_tail = pos_tail + pos_land[k, 1]
    wanted = jnp.concatenate(
        [pos_land[k, 0] for k in range(plane)] + [pos_tail[:, : plane * unit]], axis=1
    )
    line = [plane * k + spot for k in range(rows)]
    ids = jnp.concatenate(
        [lax.broadcasted_iota(jnp.int32, (base, 1), 0) + offset_of(device) for device in line]
        + [
            lax.broadcasted_iota(jnp.int32, (unit, 1), 0) + offset_of(source) + tail_row(device)
            for device in line
        ],
        axis=0,
    ).astype(F32)
    scores[...] = score_scale * dot(all_p[...], all_q[...], 1, 1)
    value = scores[...]
    hit = ids == wanted
    top = jnp.max(value, axis=0, keepdims=True)
    stat_land[spot, 0:1] = top
    stat_land[spot, 1:2] = jnp.sum(jnp.exp(value - top), axis=0, keepdims=True)
    stat_land[spot, 2:3] = jnp.sum(jnp.where(hit, value, 0.0), axis=0, keepdims=True)
    stat_land[spot, 3:4] = jnp.zeros_like(top)
    stat_group = groups.new()
    for device in plane_peers:
        stat_group.start(stat_land.at[spot], stat_land.at[spot], device)
    stat_group.done(stat_land.at[pl.ds(0, plane - 1)])
    stats = stat_land[...]
    tops = stats[:, 0]
    row_top = jnp.max(tops, axis=0, keepdims=True)
    mass = jnp.sum(stats[:, 1] * jnp.exp(tops - row_top), axis=0, keepdims=True)
    log_norm = row_top + jnp.log(mass)
    found = jnp.sum(stats[:, 2], axis=0, keepdims=True)
    loss_land[row] = jnp.broadcast_to(
        jnp.sum(log_norm - found, axis=1, keepdims=True), loss_land.shape[1:]
    )
    grads_t = (jnp.exp(scores[...] - log_norm) - hit.astype(F32)).astype(BF16)

    def scatter(part, own_base, own_tail, out_base, out_tail, land_base, land_tail, mine, peers):
        split = own_base.shape[0] * base
        own_base[...] = part[:split].reshape(own_base.shape)
        own_tail[...] = part[split:].reshape(own_tail.shape)
        out_base[...] = own_base[...].astype(out_base.dtype)
        out_tail[...] = own_tail[...].astype(out_tail.dtype)
        base_group, tail_group = groups.new(), groups.new()
        for there, device in peers:
            base_group.start(out_base.at[there], land_base.at[mine], device)
            tail_group.start(out_tail.at[there], land_tail.at[mine], device)

        def finish():
            base_group.done(land_base.at[pl.ds(0, len(peers))])
            tail_group.done(land_tail.at[pl.ds(0, len(peers))])

        return finish

    def gathered(own_part, land, mine, members):
        total = own_part[mine]
        for k in range(1, members):
            total = total + land[lax.rem(mine + k, members)].astype(F32)
        return total.astype(BF16)

    finish_dq = scatter(
        score_scale * dot(grads_t, all_p[...], 0, 0),
        dq_own_base,
        dq_own_tail,
        dq_out_base,
        dq_out_tail,
        dq_land_base,
        dq_land_tail,
        spot,
        [(lax.rem(spot + k, plane), plane_peers[k - 1]) for k in range(1, plane)],
    )
    finish_dp = scatter(
        score_scale * dot(grads_t, all_q[...], 1, 0),
        dp_own_base,
        dp_own_tail,
        dp_out_base,
        dp_out_tail,
        dp_land_base,
        dp_land_tail,
        row,
        [(lax.rem(row + k, rows), line_peers[k - 1]) for k in range(1, rows)],
    )
    loss_group = groups.new()
    for device in line_peers:
        loss_group.start(loss_land.at[row], loss_land.at[row], device)
    pair_base.done(feat_base.at[0])
    pair_tail.done(feat_tail.at[0])
    x_rows = 4 * base
    all_x[:x_rows] = feat_base[...].reshape(x_rows, width)
    all_x[x_rows:] = flat_rows(feat_tail[...])
    for t in range(TILES):
        start = pl.multiple_of(core * hidden_half + t * tile, 128)
        hidden, slope = gelu_and_slope(dot(all_x[...], w_first[:, pl.ds(start, tile)], 1, 0))
        all_hidden[t] = hidden.astype(BF16)
        all_slope[t] = slope
    finish_dq()
    de_base[core, 0] = gathered(dq_own_base, dq_land_base, spot, plane)
    de_tail[core, 0] = gathered(dq_own_tail, dq_land_tail, spot, plane)

    def send_de(side):
        base_group, tail_group = groups.new(), groups.new()
        base_group.start(de_base.at[core, side], de_base.at[core, side], partner)
        tail_group.start(de_tail.at[core, side], de_tail.at[core, side], partner)

        def finish():
            base_group.done(de_base.at[0, side])
            tail_group.done(de_tail.at[0, side])

        return finish

    finish_pair = [send_de(0)]
    finish_dp()
    de_base[core, 1] = gathered(dp_own_base, dp_land_base, row, rows)
    de_tail[core, 1] = gathered(dp_own_tail, dp_land_tail, row, rows)
    finish_pair.append(send_de(1))
    loss_group.done(loss_land.at[pl.ds(0, rows - 1)])
    loss = loss_land[0]
    for k in range(1, rows):
        loss = loss + loss_land[k]
    out_loss[...] = loss * (1.0 / (size * spare))

    low_count, high_count = 2, lanes // 2
    low_lane, high_lane = lax.rem(lane, low_count), lax.div(lane, low_count)
    low_others = [lax.rem(low_lane + k, low_count) for k in range(1, low_count)]
    high_others = [lax.rem(high_lane + k, high_count) for k in range(1, high_count)]
    skip, skip_two = half * lanes, half * high_count

    def in_plane(high, low):
        return plane * row + 2 * (high * low_count + low) + core

    def first_stage(chunk_at, part):
        t, cols = chunk_at
        for i in range(per_tile):
            for high in range(high_count):
                for low in range(low_count):
                    for j in range(2):
                        at = (((i * high_count + high) * low_count + low) * 2 + j) * chunk
                        piece = part[at : at + chunk]
                        step = t * per_tile + i
                        own[step, j, high, low, :, cols] = piece
                        if j == 0:
                            slot = (low * half + step) * high_count + high
                        else:
                            slot = skip + (high * half + step) * low_count + low
                        outgoing[slot, :, cols] = piece.astype(BF16)
        group = groups.new()
        span = per_tile * high_count
        for low in low_others:
            group.start(
                outgoing.at[pl.ds((low * half + t * per_tile) * high_count, span), :, cols],
                landing.at[pl.ds((low_lane * half + t * per_tile) * high_count, span), :, cols],
                in_plane(high_lane, low),
            )
        span = per_tile * low_count
        for high in high_others:
            group.start(
                outgoing.at[pl.ds(skip + (high * half + t * per_tile) * low_count, span), :, cols],
                landing.at[pl.ds(skip + (high_lane * half + t * per_tile) * low_count, span), :, cols],
                in_plane(high, low_lane),
            )
        return group

    def second_stage(chunk_at, before):
        t, cols = chunk_at
        count = (low_count - 1) * high_count + (high_count - 1) * low_count
        before.done(landing.at[pl.ds(0, per_tile * count), :, cols])
        for i in range(t * per_tile, (t + 1) * per_tile):
            for high in range(high_count):
                total = own[i, 0, high, low_lane, :, cols]
                for low in low_others:
                    total = total + landing[(low * half + i) * high_count + high, :, cols].astype(F32)
                own[i, 0, high, low_lane, :, cols] = total
                outgoing_two[high * half + i, :, cols] = total.astype(BF16)
            for low in range(low_count):
                total = own[i, 1, high_lane, low, :, cols]
                for high in high_others:
                    slot = skip + (high * half + i) * low_count + low
                    total = total + landing[slot, :, cols].astype(F32)
                own[i, 1, high_lane, low, :, cols] = total
                outgoing_two[skip_two + low * half + i, :, cols] = total.astype(BF16)
        group = groups.new()
        block = t * per_tile
        for high in high_others:
            group.start(
                outgoing_two.at[pl.ds(high * half + block, per_tile), :, cols],
                landing_two.at[pl.ds(high_lane * half + block, per_tile), :, cols],
                in_plane(high, low_lane),
            )
        for low in low_others:
            group.start(
                outgoing_two.at[pl.ds(skip_two + low * half + block, per_tile), :, cols],
                landing_two.at[pl.ds(skip_two + low_lane * half + block, per_tile), :, cols],
                in_plane(high_lane, low),
            )
        return group

    def line_copy(i, j, cols):
        return pltpu.make_async_remote_copy(
            src_ref=forward.at[i, j, :, cols],
            dst_ref=landed.at[row, :, cols],
            send_sem=line_send.at[i, j],
            recv_sem=line_recv.at[row],
            device_id=(plane * (half * core + i) + column + j,),
            device_id_type=MESH,
        )

    def third_stage(chunk_at, before):
        t, cols = chunk_at
        count = low_count - 1 + high_count - 1
        before.done(landing_two.at[pl.ds(0, per_tile * count), :, cols])
        for i in range(t * per_tile, (t + 1) * per_tile):
            for j in range(2):
                total = own[i, j, high_lane, low_lane, :, cols]
                if j == 0:
                    slots = [high * half + i for high in high_others]
                else:
                    slots = [skip_two + low * half + i for low in low_others]
                for slot in slots:
                    total = total + landing_two[slot, :, cols].astype(F32)
                sums[i, j, :, cols] = total
                forward[i, j, :, cols] = total.astype(BF16)

                @pl.when(plane * (half * core + i) + column + j != me)
                def _():
                    line_copy(i, j, cols).start()

    for finish in finish_pair:
        finish()
    de = jnp.concatenate([de_base[...].reshape(x_rows, embed), flat_rows(de_tail[...])], axis=0)
    act_grads = {}

    def part_of(chunk_at):
        t, cols = chunk_at
        if cols.start >= width:
            return dot(all_hidden[t], de[:, cols.start - width : cols.start - width + cols.size], 0, 0)
        if t not in act_grads:
            start = pl.multiple_of(core * hidden_half + t * tile, 128)
            back = dot(de, w_second[pl.ds(start, tile), :], 1, 1)
            act_grads[t] = (all_slope[t] * back).astype(BF16)
        return dot(act_grads[t], all_x[:, cols], 0, 0)

    piece = embed
    chunks = []
    for t in range(TILES):
        chunks.append((t, pl.ds(width, piece)))
        for low in range(0, width, piece):
            chunks.append((t, pl.ds(low, piece)))
    ones, twos = [], []
    for at in range(len(chunks) + DELAY):
        if at < len(chunks):
            for ahead in range(len(ones), min(at + AHEAD, len(chunks))):
                ones.append(first_stage(chunks[ahead], part_of(chunks[ahead])))
            twos.append(second_stage(chunks[at], ones[at]))
        if at >= DELAY:
            third_stage(chunks[at - DELAY], twos[at - DELAY])

    sender_core = lax.div(row, half)
    whole = pl.ds(0, width + embed)
    for i in range(half):
        for j in range(2):

            @pl.when(plane * (half * core + i) + column + j != me)
            def _():
                line_copy(i, j, whole).wait_send()

    for sender_row in range(rows):
        sender = plane * sender_row + column + sender_core

        @pl.when(sender != me)
        def _():
            pltpu.make_async_remote_copy(
                src_ref=forward.at[0, 0],
                dst_ref=landed.at[sender_row],
                send_sem=line_send.at[0, 0],
                recv_sem=line_recv.at[sender_row],
                device_id=(sender,),
                device_id_type=MESH,
            ).wait_recv()

    total = jnp.where(sender_core == core, sums[lax.rem(row, half), core], 0.0)
    for sender_row in range(rows):
        sender = plane * sender_row + column + sender_core
        total = total + jnp.where(sender == me, 0.0, landed[sender_row].astype(F32))
    out_all[...] = total


def split_kernel(loss, total, mean_loss, first, second):
    width = first.shape[1]
    mean_loss[0] = loss[0, 0]
    first[...] = total[:, :width]
    second[...] = total[:, width:]


def split_outputs(loss, total, width):
    vmem = pl.BlockSpec(memory_space=pltpu.VMEM)
    chunk, across = total.shape
    return pl.pallas_call(
        split_kernel,
        out_shape=[
            jax.ShapeDtypeStruct((1,), F32),
            jax.ShapeDtypeStruct((chunk, width), F32),
            jax.ShapeDtypeStruct((chunk, across - width), F32),
        ],
        in_specs=[pl.BlockSpec(memory_space=pltpu.SMEM), vmem],
        out_specs=[pl.BlockSpec(memory_space=pltpu.SMEM), vmem, vmem],
    )(loss, total)


def step(size, plane, score_scale, counts, *arrays):
    query_features, _, positives, w_first, w_second = arrays
    rows, lanes = size // plane, plane // 2
    half = rows // 2
    width, hidden_width = w_first.shape
    embed = w_second.shape[1]
    chunk = hidden_width // size
    across = width + embed
    base = query_features.shape[0] // 2
    unit = base // 16
    block = base + unit
    vmem = pl.BlockSpec(memory_space=pltpu.VMEM)
    anywhere = pl.BlockSpec(memory_space=pl.ANY)
    count = 20 + 2 * TILES * (1 + width // embed)

    def split(members, dtype):
        return [
            pltpu.VMEM((members, base, embed), dtype),
            pltpu.VMEM((members, unit, embed), dtype),
        ]

    scratch = [
        pltpu.VMEM((rows, 16 // rows, unit, 2 * width), BF16),
        pltpu.VMEM((16 // rows, rows, unit, 2 * width), BF16),
        pltpu.VMEM((rows, unit, 2 * width), BF16),
        pltpu.VMEM((rows, unit, 2 * width), BF16),
        pltpu.VMEM((16,) + positives.shape, F32),
        pltpu.VMEM((2, 2, base, width), BF16),
        pltpu.VMEM((2, 2, unit, width), BF16),
        *split(plane, BF16),
        *split(rows, BF16),
        pltpu.VMEM((plane, 2, 1, base), F32),
        pltpu.VMEM((plane * block, embed), BF16),
        pltpu.VMEM((rows * block, embed), BF16),
        pltpu.VMEM((rows * block, plane * block), F32),
        pltpu.VMEM((plane, 4, plane * block), F32),
        *split(plane, F32),
        *split(plane, BF16),
        *split(plane, BF16),
        *split(rows, F32),
        *split(rows, BF16),
        *split(rows, BF16),
        pltpu.VMEM((rows, 8, 128), F32),
        pltpu.VMEM((2, 2, base, embed), BF16),
        pltpu.VMEM((2, 2, unit, embed), BF16),
        pltpu.VMEM((2, unit, width), BF16),
        pltpu.VMEM((4 * block, width), BF16),
        pltpu.VMEM((half, 2, lanes // 2, 2, chunk, across), F32),
        pltpu.VMEM((2 * half * lanes, chunk, across), BF16),
        pltpu.VMEM((2 * half * lanes, chunk, across), BF16),
        pltpu.VMEM((half * (lanes // 2 + 2), chunk, across), BF16),
        pltpu.VMEM((half * (lanes // 2 + 2), chunk, across), BF16),
        pltpu.VMEM((half, 2, chunk, across), F32),
        pltpu.VMEM((half, 2, chunk, across), BF16),
        pltpu.VMEM((rows, chunk, across), BF16),
        pltpu.SemaphoreType.DMA((count,)),
        pltpu.SemaphoreType.DMA((count,)),
        pltpu.SemaphoreType.DMA((half, 2)),
        pltpu.SemaphoreType.DMA((rows,)),
        pltpu.VMEM(w_first.shape, BF16),
        pltpu.VMEM(w_second.shape, BF16),
        pltpu.VMEM((TILES, 4 * block, hidden_width // 2 // TILES), BF16),
        pltpu.VMEM((TILES, 4 * block, hidden_width // 2 // TILES), F32),
        pltpu.SemaphoreType.DMA((8,)),
    ]
    return pl.pallas_call(
        functools.partial(step_kernel, size, plane, score_scale),
        out_shape=[
            jax.ShapeDtypeStruct((8, 128), F32),
            jax.ShapeDtypeStruct((chunk, across), F32),
        ],
        in_specs=[pl.BlockSpec(memory_space=pltpu.SMEM)] + [anywhere] * 2 + [vmem]
        + [anywhere] * 2,
        out_specs=[vmem] * 2,
        scratch_shapes=scratch,
        compiler_params=pltpu.CompilerParams(
            collective_id=0, has_side_effects=True, vmem_limit_bytes=60 * 1024 * 1024
        ),
    )(counts, *arrays)


def body(query_features, passage_features, counts, positives, w_first, w_second):
    device_count = lax.axis_size("dp")
    plane = 1 << device_count.bit_length() // 2
    score_scale = 2.5 * w_second.shape[1] ** (-0.5)
    loss, total = step(
        device_count,
        plane,
        score_scale,
        counts,
        query_features,
        passage_features,
        positives[None, :],
        w_first,
        w_second,
    )
    mean_loss, grad_first, grad_second = split_outputs(loss, total, w_first.shape[0])
    return (mean_loss[0], grad_first.T, grad_second)


def solution(mesh):
    return jax.shard_map(
        body,
        mesh=mesh,
        in_specs=(P("dp", None), P("dp", None), P(), P("dp"), P(), P()),
        out_specs=(P(), P(None, "dp"), P("dp", None)),
        check_vma=False,
    )
```

```python
import functools

import jax
import jax.numpy as jnp
from jax import lax
from jax.experimental import pallas as pl
from jax.experimental.pallas import tpu as pltpu
from jax.sharding import PartitionSpec as P

MESH = pl.DeviceIdType.MESH
F32 = jnp.float32
BF16 = jnp.bfloat16
GELU_ROOT = 0.7978845608028654
GELU_CUBE = 0.044715
TILES = 2
AHEAD = 3
DELAY = 2


def gelu_and_slope(value):
    square = value * value
    bent = jnp.tanh(GELU_ROOT * value * (1.0 + GELU_CUBE * square))
    rise = 0.5 * (1.0 + bent)
    slope = rise + 0.5 * value * (1.0 - bent * bent) * (
        GELU_ROOT * (1.0 + 3.0 * GELU_CUBE * square)
    )
    return value * rise, slope


def dot(left, right, left_dim, right_dim):
    return lax.dot_general(
        left, right, (((left_dim,), (right_dim,)), ((), ())), preferred_element_type=F32
    )


def flat_rows(blocks):
    return blocks.astype(F32).reshape(-1, blocks.shape[-1]).astype(BF16)


class Group:
    def __init__(self, send, recv):
        self.send, self.recv = send, recv

    def start(self, source, landing, device):
        pltpu.make_async_remote_copy(
            src_ref=source,
            dst_ref=landing,
            send_sem=self.send,
            recv_sem=self.recv,
            device_id=(device,),
            device_id_type=MESH,
        ).start()

    def landed(self, span):
        pltpu.make_async_copy(span, span, self.recv).wait()

    def sent(self, span):
        pltpu.make_async_copy(span, span, self.send).wait()

    def done(self, span):
        self.landed(span)
        self.sent(span)


class Groups:
    def __init__(self, send, recv):
        self.send, self.recv, self.used = send, recv, 0

    def new(self):
        self.used += 1
        return Group(self.send.at[self.used - 1], self.recv.at[self.used - 1])


def step_kernel(
    size,
    plane,
    score_scale,
    counts,
    query_hbm,
    passage_hbm,
    positives,
    w_first_hbm,
    w_second_hbm,
    out_loss,
    out_all,
    units,
    unit_mid,
    unit_pass,
    unit_land,
    unit_pos,
    feat_base,
    feat_tail,
    q_base,
    q_tail,
    p_base,
    q_unit,
    q_unit_land,
    p_tails,
    pos_land,
    all_q,
    all_p,
    scores,
    stat_land,
    found_land,
    dq_own_base,
    dq_own_tail,
    dq_out_base,
    dq_out_tail,
    dq_land_base,
    dq_land_tail,
    dp_own_base,
    dp_own_tail,
    dp_out_base,
    dp_out_tail,
    dp_land_base,
    dp_land_tail,
    loss_land,
    de_base,
    de_tail,
    all_x,
    own,
    outgoing,
    landing,
    outgoing_two,
    landing_two,
    sums,
    forward,
    landed,
    send_sems,
    recv_sems,
    line_send,
    line_recv,
    w_first,
    w_second,
    all_hidden,
    all_slope,
    load_sems,
):
    me = lax.axis_index("dp")
    rows = size // plane
    half = rows // 2
    lanes = plane // 2
    stride = size // 16
    row = lax.div(me, plane)
    spot = lax.rem(me, plane)
    core = lax.rem(me, 2)
    lane = lax.div(spot, 2)
    column = spot - core
    place = lax.div(me, stride)
    partner = me + 1 - 2 * core
    width, hidden_width = w_first.shape
    embed = w_second.shape[1]
    base = q_base.shape[1]
    unit = q_tail.shape[1]
    hidden_half = hidden_width // 2
    tile = hidden_half // TILES
    per_tile = half // TILES
    chunk = hidden_half // (half * lanes * 2)
    groups = Groups(send_sems, recv_sems)

    plane_peers = [row * plane + lax.rem(spot + k, plane) for k in range(1, plane)]
    line_peers = [lax.rem(row + k, rows) * plane + spot for k in range(1, rows)]
    bits = [1 << at for at in range(lanes.bit_length() - 1)]
    lane_others = []
    for flips in range(1, lanes):
        away = lane
        for bit in bits:
            if flips & bit:
                away = away + bit - 2 * bit * lax.rem(lax.div(lane, bit), 2)
        lane_others.append(away)
    barrier = pltpu.get_barrier_semaphore()

    def greet(device):
        pl.semaphore_signal(barrier, inc=1, device_id=(device,), device_id_type=MESH)

    for k in range(1, 16):
        greet(lax.rem(place + k, 16) * stride + lax.rem(me, stride))
    for device in plane_peers:
        greet(device)
    in_column = 2 * row + core
    for k in range(1, 2 * rows):
        other = lax.rem(in_column + k, 2 * rows)
        greet(plane * lax.div(other, 2) + column + lax.rem(other, 2))

    spare = base + unit
    near = plane // stride
    aside = lax.div(spot, stride)
    for at, (features, sem) in enumerate(((query_hbm, 0), (passage_hbm, 1))):
        side = pl.ds(at * width, width)
        for u in range(15):
            there = u + lax.div(u + 16 - place, 16)
            pltpu.make_async_copy(
                features.at[pl.ds(spare + u * unit, unit), :],
                units.at[lax.div(there, near), lax.rem(there, near), :, side],
                load_sems.at[sem],
            ).start()
        pltpu.make_async_copy(
            features.at[pl.ds(base, unit), :], units.at[row, aside, :, side], load_sems.at[sem]
        ).start()
    base_loads = [
        pltpu.make_async_copy(
            features.at[pl.ds(0, base), :], feat_base.at[core, at], load_sems.at[2 + at]
        )
        for at, features in enumerate((query_hbm, passage_hbm))
    ]
    weight_loads = [
        pltpu.make_async_copy(w_first_hbm, w_first, load_sems.at[4]),
        pltpu.make_async_copy(w_second_hbm, w_second, load_sems.at[5]),
    ]
    for load in base_loads + weight_loads:
        load.start()
    unit_pos[place] = positives[...].astype(F32)

    pl.semaphore_wait(barrier, 15 + plane - 1 + 2 * rows - 1)
    for features, sem in ((query_hbm, 0), (passage_hbm, 1)):
        extra = features.at[pl.ds(base, 16 * unit), :]
        pltpu.make_async_copy(extra, extra, load_sems.at[sem]).wait()

    mid_group = groups.new()
    for k in range(1, near):
        there = lax.rem(aside + k, near)
        mid_group.start(
            units.at[:, there],
            unit_mid.at[aside],
            row * plane + there * stride + lax.rem(me, stride),
        )
    where_group = groups.new()
    for k in range(1, 16):
        device = lax.rem(place + k, 16) * stride + lax.rem(me, stride)
        where_group.start(unit_pos.at[place], unit_pos.at[place], device)

    heavies = []
    for g in range(stride):
        at = jnp.int32(0)
        for k in range(16):
            at = at + jnp.where(counts[g + stride * k] > base, g + stride * k, 0)
        heavies.append(at)
    source = jnp.int32(0)
    for g in range(stride):
        source = source + jnp.where(lax.rem(me, stride) == g, heavies[g], 0)
    heavy_place = jnp.int32(0)
    for k in range(16):
        heavy_place = heavy_place + jnp.where(source >= stride * (k + 1), 1, 0)

    def offset_of(device):
        before = jnp.int32(0)
        for at in heavies:
            before = before + jnp.where(at < device, 1, 0)
        return base * (device + before)

    def tail_row(device):
        piece = lax.div(device, stride) - jnp.where(source < device, 1, 0)
        return jnp.where(source == device, base, spare + unit * piece)

    def tower(features):
        total = None
        for low in range(0, hidden_width, tile):
            act = dot(features, w_first[:, low : low + tile], 1, 0)
            hidden = gelu_and_slope(act)[0].astype(BF16)
            part = dot(hidden, w_second[low : low + tile, :], 1, 0)
            total = part if total is None else total + part
        return total.astype(BF16)

    for load in base_loads:
        load.wait()
    pair_base = groups.new()
    pair_base.start(feat_base.at[core], feat_base.at[core], partner)
    for load in weight_loads:
        load.wait()
    p_base[row] = tower(feat_base[core, 1])
    p_groups = [groups.new() for _ in range(rows)]
    relayed = rows == 4
    if relayed:

        def p_send(block, there, group):
            group.start(p_base.at[block], p_base.at[block], there * plane + spot)

        for at, order in enumerate(((2, 1), (3, 2, 0), (0, 1, 3), (1, 2))):

            @pl.when(row == at)
            def _():
                for there in order:
                    p_send(at, there, p_groups[at])
    else:
        for k in range(1, rows):
            p_groups[k].start(p_base.at[row], p_base.at[row], line_peers[k - 1])
    q_base[spot] = tower(feat_base[core, 0])
    q_pair = groups.new()
    q_pair.start(q_base.at[spot], q_base.at[spot], partner)
    q_groups = []
    for away in lane_others:
        group = groups.new()
        group.start(q_base.at[spot], q_base.at[spot], row * plane + 2 * away + core)
        q_groups.append(group)

    mid_group.done(unit_mid.at[pl.ds(0, near - 1)])
    source_row, source_aside = jnp.int32(0), heavy_place
    for k in range(1, rows):
        beyond = heavy_place >= k * near
        source_row = source_row + jnp.where(beyond, 1, 0)
        source_aside = source_aside - jnp.where(beyond, near, 0)
    passed = jnp.where(
        source_aside == aside, units[:, aside].astype(F32), unit_mid[source_aside].astype(F32)
    )
    unit_pass[...] = passed.astype(BF16)
    tails = rows * unit
    mid_x = jnp.concatenate(
        [passed[:, :, :width].reshape(tails, width), passed[:, :, width:].reshape(tails, width)],
        axis=0,
    ).astype(BF16)
    mid_e = tower(mid_x)
    q_unit[...] = mid_e[:tails].astype(F32).reshape(rows, unit, embed).astype(BF16)
    p_tails[row] = mid_e[tails:]
    q_unit_group, p_tail_group, pass_group = groups.new(), groups.new(), groups.new()
    for k in range(1, rows):
        there = lax.rem(row + k, rows)
        q_unit_group.start(q_unit.at[there], q_unit_land.at[row], there * plane + spot)
    for device in line_peers:
        p_tail_group.start(p_tails.at[row], p_tails.at[row], device)

    where_group.done(unit_pos.at[pl.ds(0, 15)])
    slots = lax.broadcasted_iota(jnp.int32, (unit, positives.shape[1]), 1)
    chosen = lax.broadcasted_iota(jnp.int32, slots.shape, 0) + tail_row(me)
    tail_pos = jnp.sum(
        jnp.where(slots == chosen, unit_pos[heavy_place], 0.0), axis=1, keepdims=True
    )
    pos_land[spot, 0] = positives[:, :base].astype(F32)
    sub = lax.broadcasted_iota(jnp.int32, (unit, base), 0) + spot * unit
    along = lax.broadcasted_iota(jnp.int32, (unit, base), 1)
    pos_land[spot, 1] = jnp.sum(jnp.where(sub == along, tail_pos, 0.0), axis=0, keepdims=True)
    pos_group = groups.new()
    for device in plane_peers:
        pos_group.start(pos_land.at[spot], pos_land.at[spot], device)

    if relayed:
        for at, (far, end) in ((1, (3, 0)), (2, (0, 3))):

            @pl.when(row == at)
            def _():
                p_groups[far].landed(p_base.at[far])
                p_send(far, end, p_groups[far])

    q_unit_group.done(q_unit_land.at[pl.ds(0, rows - 1)])
    q_tail[spot] = jnp.where(
        source_row == row, q_unit[row].astype(F32), q_unit_land[source_row].astype(F32)
    ).astype(BF16)
    q_tail_group = groups.new()
    for device in plane_peers:
        q_tail_group.start(q_tail.at[spot], q_tail.at[spot], device)
    for k in range(1, rows):
        there = lax.rem(row + k, rows)
        pass_group.start(unit_pass.at[there], unit_land.at[row], there * plane + spot)

    for away, group in zip(lane_others, q_groups):
        there = 2 * away + core
        group.done(q_base.at[there])
        q_pair.start(q_base.at[there], q_base.at[there], partner)
    if relayed:
        for at in range(rows):
            early = {0: 2, 3: 1}.get(at, at)

            @pl.when(jnp.logical_and(row != at, row != early))
            def _():
                p_groups[at].landed(p_base.at[at])
    else:
        for k in range(1, rows):
            p_groups[k].done(p_base.at[lax.rem(row + rows - k, rows)])
    q_pair.done(q_base.at[pl.ds(0, lanes)])

    q_rows, p_rows = plane * base, rows * base
    line = [plane * k + spot for k in range(rows)]
    base_ids = jnp.concatenate(
        [lax.broadcasted_iota(jnp.int32, (base, 1), 0) + offset_of(device) for device in line],
        axis=0,
    ).astype(F32)
    tail_ids = jnp.concatenate(
        [
            lax.broadcasted_iota(jnp.int32, (unit, 1), 0) + offset_of(source) + tail_row(device)
            for device in line
        ],
        axis=0,
    ).astype(F32)
    all_q[:q_rows] = q_base[...].reshape(q_rows, embed)
    all_p[:p_rows] = p_base[...].reshape(p_rows, embed)
    pos_group.done(pos_land.at[pl.ds(0, plane - 1)])
    base_wanted = jnp.concatenate([pos_land[k, 0] for k in range(plane)], axis=1)

    def spread(value, ids, wanted):
        top = jnp.max(value, axis=0, keepdims=True)
        mass = jnp.sum(jnp.exp(value - top), axis=0, keepdims=True)
        return top, mass, jnp.sum(jnp.where(ids == wanted, value, 0.0), axis=0, keepdims=True)

    def merge(one, two):
        top = jnp.maximum(one[0], two[0])
        mass = one[1] * jnp.exp(one[0] - top) + two[1] * jnp.exp(two[0] - top)
        return top, mass, one[2] + two[2]

    def scored(p_part, q_part):
        scores[p_part, q_part] = score_scale * dot(all_p[p_part], all_q[q_part], 1, 1)
        return scores[p_part, q_part]

    p_base_part, p_tail_part = slice(0, p_rows), slice(p_rows, all_p.shape[0])
    q_base_part, q_tail_part = slice(0, q_rows), slice(q_rows, all_q.shape[0])
    base_stats = spread(scored(p_base_part, q_base_part), base_ids, base_wanted)

    p_tail_group.done(p_tails.at[pl.ds(0, rows - 1)])
    all_p[p_rows:] = p_tails[source_row]
    base_stats = merge(
        base_stats, spread(scored(p_tail_part, q_base_part), tail_ids, base_wanted)
    )
    q_tail_group.done(q_tail.at[pl.ds(0, plane - 1)])
    all_q[q_rows:] = flat_rows(q_tail[...])
    pos_tail = pos_land[0, 1]
    for k in range(1, plane):
        pos_tail = pos_tail + pos_land[k, 1]
    tail_wanted = pos_tail[:, : plane * unit]
    ids = jnp.concatenate([base_ids, tail_ids], axis=0)
    tail_stats = spread(scored(slice(0, all_p.shape[0]), q_tail_part), ids, tail_wanted)
    stat_land[spot, 0:1, :q_rows] = base_stats[0]
    stat_land[spot, 0:1, q_rows:] = tail_stats[0]
    stat_land[spot, 1:2, :q_rows] = base_stats[1]
    stat_land[spot, 1:2, q_rows:] = tail_stats[1]
    found_land[spot, :, :q_rows] = base_stats[2]
    found_land[spot, :, q_rows:] = tail_stats[2]
    wanted = jnp.concatenate([base_wanted, tail_wanted], axis=1)
    hit = ids == wanted
    stat_group, found_group = groups.new(), groups.new()
    for device in plane_peers:
        stat_group.start(stat_land.at[spot], stat_land.at[spot], device)
    for device in plane_peers:
        found_group.start(found_land.at[spot], found_land.at[spot], device)
    pass_group.done(unit_land.at[pl.ds(0, rows - 1)])
    got = jnp.where(
        source_row == row, unit_pass[row].astype(F32), unit_land[source_row].astype(F32)
    )
    feat_tail[core, 0] = got[:, :width].astype(BF16)
    feat_tail[core, 1] = got[:, width:].astype(BF16)
    pair_tail = groups.new()
    pair_tail.start(feat_tail.at[core], feat_tail.at[core], partner)
    stat_group.done(stat_land.at[pl.ds(0, plane - 1)])
    stats = stat_land[...]
    tops = stats[:, 0]
    row_top = jnp.max(tops, axis=0, keepdims=True)
    mass = jnp.sum(stats[:, 1] * jnp.exp(tops - row_top), axis=0, keepdims=True)
    log_norm = row_top + jnp.log(mass)
    grads_t = (jnp.exp(scores[...] - log_norm) - hit.astype(F32)).astype(BF16)

    def scatter(part, own_base, own_tail, out_base, out_tail, land_base, land_tail, mine, peers):
        split = own_base.shape[0] * base
        own_base[...] = part[:split].reshape(own_base.shape)
        own_tail[...] = part[split:].reshape(own_tail.shape)
        out_base[...] = own_base[...].astype(out_base.dtype)
        out_tail[...] = own_tail[...].astype(out_tail.dtype)
        base_group, tail_group = groups.new(), groups.new()
        for there, device in peers:
            base_group.start(out_base.at[there], land_base.at[mine], device)
            tail_group.start(out_tail.at[there], land_tail.at[mine], device)

        def finish():
            base_group.done(land_base.at[pl.ds(0, len(peers))])
            tail_group.done(land_tail.at[pl.ds(0, len(peers))])

        return finish

    def gathered(own_part, land, mine, members):
        total = own_part[mine]
        for k in range(1, members):
            total = total + land[lax.rem(mine + k, members)].astype(F32)
        return total.astype(BF16)

    finish_dq = scatter(
        score_scale * dot(grads_t, all_p[...], 0, 0),
        dq_own_base,
        dq_own_tail,
        dq_out_base,
        dq_out_tail,
        dq_land_base,
        dq_land_tail,
        spot,
        [(lax.rem(spot + k, plane), plane_peers[k - 1]) for k in range(1, plane)],
    )
    finish_dp = scatter(
        score_scale * dot(grads_t, all_q[...], 1, 0),
        dp_own_base,
        dp_own_tail,
        dp_out_base,
        dp_out_tail,
        dp_land_base,
        dp_land_tail,
        row,
        [(lax.rem(row + k, rows), line_peers[k - 1]) for k in range(1, rows)],
    )
    found_group.done(found_land.at[pl.ds(0, plane - 1)])
    found = jnp.sum(found_land[...][:, 0], axis=0, keepdims=True)
    loss_land[row] = jnp.broadcast_to(
        jnp.sum(log_norm - found, axis=1, keepdims=True), loss_land.shape[1:]
    )
    loss_group = groups.new()
    for device in line_peers:
        loss_group.start(loss_land.at[row], loss_land.at[row], device)
    pair_base.done(feat_base.at[0])
    pair_tail.done(feat_tail.at[0])
    x_rows = 4 * base
    all_x[:x_rows] = feat_base[...].reshape(x_rows, width)
    all_x[x_rows:] = flat_rows(feat_tail[...])
    for t in range(TILES):
        start = pl.multiple_of(core * hidden_half + t * tile, 128)
        hidden, slope = gelu_and_slope(dot(all_x[...], w_first[:, pl.ds(start, tile)], 1, 0))
        all_hidden[t] = hidden.astype(BF16)
        all_slope[t] = slope
    finish_dq()
    de_base[core, 0] = gathered(dq_own_base, dq_land_base, spot, plane)
    de_tail[core, 0] = gathered(dq_own_tail, dq_land_tail, spot, plane)

    def send_de(side):
        base_group, tail_group = groups.new(), groups.new()
        base_group.start(de_base.at[core, side], de_base.at[core, side], partner)
        tail_group.start(de_tail.at[core, side], de_tail.at[core, side], partner)

        def finish():
            base_group.done(de_base.at[0, side])
            tail_group.done(de_tail.at[0, side])

        return finish

    finish_pair = [send_de(0)]
    finish_dp()
    de_base[core, 1] = gathered(dp_own_base, dp_land_base, row, rows)
    de_tail[core, 1] = gathered(dp_own_tail, dp_land_tail, row, rows)
    finish_pair.append(send_de(1))
    loss_group.done(loss_land.at[pl.ds(0, rows - 1)])
    loss = loss_land[0]
    for k in range(1, rows):
        loss = loss + loss_land[k]
    out_loss[...] = loss * (1.0 / (size * spare))

    low_count, high_count = 2, lanes // 2
    low_lane, high_lane = lax.rem(lane, low_count), lax.div(lane, low_count)
    low_others = [lax.rem(low_lane + k, low_count) for k in range(1, low_count)]
    high_others = [lax.rem(high_lane + k, high_count) for k in range(1, high_count)]
    skip, skip_two = half * lanes, half * high_count

    def in_plane(high, low):
        return plane * row + 2 * (high * low_count + low) + core

    def first_stage(chunk_at, part):
        t, cols = chunk_at
        for i in range(per_tile):
            for high in range(high_count):
                for low in range(low_count):
                    for j in range(2):
                        at = (((i * high_count + high) * low_count + low) * 2 + j) * chunk
                        piece = part[at : at + chunk]
                        step = t * per_tile + i
                        own[step, j, high, low, :, cols] = piece
                        if j == 0:
                            slot = (low * half + step) * high_count + high
                        else:
                            slot = skip + (high * half + step) * low_count + low
                        outgoing[slot, :, cols] = piece.astype(BF16)
        group = groups.new()
        span = per_tile * high_count
        for low in low_others:
            group.start(
                outgoing.at[pl.ds((low * half + t * per_tile) * high_count, span), :, cols],
                landing.at[pl.ds((low_lane * half + t * per_tile) * high_count, span), :, cols],
                in_plane(high_lane, low),
            )
        span = per_tile * low_count
        for high in high_others:
            group.start(
                outgoing.at[pl.ds(skip + (high * half + t * per_tile) * low_count, span), :, cols],
                landing.at[pl.ds(skip + (high_lane * half + t * per_tile) * low_count, span), :, cols],
                in_plane(high, low_lane),
            )
        return group

    def second_stage(chunk_at, before):
        t, cols = chunk_at
        count = (low_count - 1) * high_count + (high_count - 1) * low_count
        before.done(landing.at[pl.ds(0, per_tile * count), :, cols])
        for i in range(t * per_tile, (t + 1) * per_tile):
            for high in range(high_count):
                total = own[i, 0, high, low_lane, :, cols]
                for low in low_others:
                    total = total + landing[(low * half + i) * high_count + high, :, cols].astype(F32)
                own[i, 0, high, low_lane, :, cols] = total
                outgoing_two[high * half + i, :, cols] = total.astype(BF16)
            for low in range(low_count):
                total = own[i, 1, high_lane, low, :, cols]
                for high in high_others:
                    slot = skip + (high * half + i) * low_count + low
                    total = total + landing[slot, :, cols].astype(F32)
                own[i, 1, high_lane, low, :, cols] = total
                outgoing_two[skip_two + low * half + i, :, cols] = total.astype(BF16)
        group = groups.new()
        block = t * per_tile
        for high in high_others:
            group.start(
                outgoing_two.at[pl.ds(high * half + block, per_tile), :, cols],
                landing_two.at[pl.ds(high_lane * half + block, per_tile), :, cols],
                in_plane(high, low_lane),
            )
        for low in low_others:
            group.start(
                outgoing_two.at[pl.ds(skip_two + low * half + block, per_tile), :, cols],
                landing_two.at[pl.ds(skip_two + low_lane * half + block, per_tile), :, cols],
                in_plane(high_lane, low),
            )
        return group

    def line_copy(i, j, cols):
        return pltpu.make_async_remote_copy(
            src_ref=forward.at[i, j, :, cols],
            dst_ref=landed.at[row, :, cols],
            send_sem=line_send.at[i, j],
            recv_sem=line_recv.at[row],
            device_id=(plane * (half * core + i) + column + j,),
            device_id_type=MESH,
        )

    def third_stage(chunk_at, before):
        t, cols = chunk_at
        count = low_count - 1 + high_count - 1
        before.done(landing_two.at[pl.ds(0, per_tile * count), :, cols])
        for i in range(t * per_tile, (t + 1) * per_tile):
            for j in range(2):
                total = own[i, j, high_lane, low_lane, :, cols]
                if j == 0:
                    slots = [high * half + i for high in high_others]
                else:
                    slots = [skip_two + low * half + i for low in low_others]
                for slot in slots:
                    total = total + landing_two[slot, :, cols].astype(F32)
                sums[i, j, :, cols] = total
                forward[i, j, :, cols] = total.astype(BF16)

                @pl.when(plane * (half * core + i) + column + j != me)
                def _():
                    line_copy(i, j, cols).start()

    for finish in finish_pair:
        finish()
    de = jnp.concatenate([de_base[...].reshape(x_rows, embed), flat_rows(de_tail[...])], axis=0)
    act_grads = {}

    def part_of(chunk_at):
        t, cols = chunk_at
        if cols.start >= width:
            return dot(all_hidden[t], de[:, cols.start - width : cols.start - width + cols.size], 0, 0)
        if t not in act_grads:
            start = pl.multiple_of(core * hidden_half + t * tile, 128)
            back = dot(de, w_second[pl.ds(start, tile), :], 1, 1)
            act_grads[t] = (all_slope[t] * back).astype(BF16)
        return dot(act_grads[t], all_x[:, cols], 0, 0)

    piece = embed
    chunks = []
    for t in range(TILES):
        chunks.append((t, pl.ds(width, piece)))
        for low in range(0, width, piece):
            chunks.append((t, pl.ds(low, piece)))
    ones, twos = [], []
    for at in range(len(chunks) + DELAY):
        if at < len(chunks):
            for ahead in range(len(ones), min(at + AHEAD, len(chunks))):
                ones.append(first_stage(chunks[ahead], part_of(chunks[ahead])))
            twos.append(second_stage(chunks[at], ones[at]))
        if at >= DELAY:
            third_stage(chunks[at - DELAY], twos[at - DELAY])

    if relayed:
        for at in range(rows):

            @pl.when(row == at)
            def _():
                p_groups[at].sent(p_base.at[pl.ds(0, 3 if at in (1, 2) else 2)])
                if at in (1, 2):
                    far = 3 if at == 1 else 0
                    p_groups[far].sent(p_base.at[far])

    sender_core = lax.div(row, half)
    whole = pl.ds(0, width + embed)
    for i in range(half):
        for j in range(2):

            @pl.when(plane * (half * core + i) + column + j != me)
            def _():
                line_copy(i, j, whole).wait_send()

    for sender_row in range(rows):
        sender = plane * sender_row + column + sender_core

        @pl.when(sender != me)
        def _():
            pltpu.make_async_remote_copy(
                src_ref=forward.at[0, 0],
                dst_ref=landed.at[sender_row],
                send_sem=line_send.at[0, 0],
                recv_sem=line_recv.at[sender_row],
                device_id=(sender,),
                device_id_type=MESH,
            ).wait_recv()

    total = jnp.where(sender_core == core, sums[lax.rem(row, half), core], 0.0)
    for sender_row in range(rows):
        sender = plane * sender_row + column + sender_core
        total = total + jnp.where(sender == me, 0.0, landed[sender_row].astype(F32))
    out_all[...] = total


def split_kernel(loss, total, mean_loss, first, second):
    width = first.shape[1]
    mean_loss[0] = loss[0, 0]
    first[...] = total[:, :width]
    second[...] = total[:, width:]


def split_outputs(loss, total, width):
    vmem = pl.BlockSpec(memory_space=pltpu.VMEM)
    chunk, across = total.shape
    return pl.pallas_call(
        split_kernel,
        out_shape=[
            jax.ShapeDtypeStruct((1,), F32),
            jax.ShapeDtypeStruct((chunk, width), F32),
            jax.ShapeDtypeStruct((chunk, across - width), F32),
        ],
        in_specs=[pl.BlockSpec(memory_space=pltpu.SMEM), vmem],
        out_specs=[pl.BlockSpec(memory_space=pltpu.SMEM), vmem, vmem],
    )(loss, total)


def step(size, plane, score_scale, counts, *arrays):
    query_features, _, positives, w_first, w_second = arrays
    rows, lanes = size // plane, plane // 2
    half = rows // 2
    width, hidden_width = w_first.shape
    embed = w_second.shape[1]
    chunk = hidden_width // size
    across = width + embed
    base = query_features.shape[0] // 2
    unit = base // 16
    block = base + unit
    vmem = pl.BlockSpec(memory_space=pltpu.VMEM)
    anywhere = pl.BlockSpec(memory_space=pl.ANY)
    count = 20 + rows + lanes + 2 * TILES * (1 + width // embed)

    def split(members, dtype):
        return [
            pltpu.VMEM((members, base, embed), dtype),
            pltpu.VMEM((members, unit, embed), dtype),
        ]

    scratch = [
        pltpu.VMEM((rows, 16 // rows, unit, 2 * width), BF16),
        pltpu.VMEM((16 // rows, rows, unit, 2 * width), BF16),
        pltpu.VMEM((rows, unit, 2 * width), BF16),
        pltpu.VMEM((rows, unit, 2 * width), BF16),
        pltpu.VMEM((16,) + positives.shape, F32),
        pltpu.VMEM((2, 2, base, width), BF16),
        pltpu.VMEM((2, 2, unit, width), BF16),
        *split(plane, BF16),
        pltpu.VMEM((rows, base, embed), BF16),
        pltpu.VMEM((rows, unit, embed), BF16),
        pltpu.VMEM((rows, unit, embed), BF16),
        pltpu.VMEM((rows, rows * unit, embed), BF16),
        pltpu.VMEM((plane, 2, 1, base), F32),
        pltpu.VMEM((plane * block, embed), BF16),
        pltpu.VMEM((rows * block, embed), BF16),
        pltpu.VMEM((rows * block, plane * block), F32),
        pltpu.VMEM((plane, 2, plane * block), F32),
        pltpu.VMEM((plane, 1, plane * block), F32),
        *split(plane, F32),
        *split(plane, BF16),
        *split(plane, BF16),
        *split(rows, F32),
        *split(rows, BF16),
        *split(rows, BF16),
        pltpu.VMEM((rows, 8, 128), F32),
        pltpu.VMEM((2, 2, base, embed), BF16),
        pltpu.VMEM((2, 2, unit, embed), BF16),
        pltpu.VMEM((4 * block, width), BF16),
        pltpu.VMEM((half, 2, lanes // 2, 2, chunk, across), F32),
        pltpu.VMEM((2 * half * lanes, chunk, across), BF16),
        pltpu.VMEM((2 * half * lanes, chunk, across), BF16),
        pltpu.VMEM((half * (lanes // 2 + 2), chunk, across), BF16),
        pltpu.VMEM((half * (lanes // 2 + 2), chunk, across), BF16),
        pltpu.VMEM((half, 2, chunk, across), F32),
        pltpu.VMEM((half, 2, chunk, across), BF16),
        pltpu.VMEM((rows, chunk, across), BF16),
        pltpu.SemaphoreType.DMA((count,)),
        pltpu.SemaphoreType.DMA((count,)),
        pltpu.SemaphoreType.DMA((half, 2)),
        pltpu.SemaphoreType.DMA((rows,)),
        pltpu.VMEM(w_first.shape, BF16),
        pltpu.VMEM(w_second.shape, BF16),
        pltpu.VMEM((TILES, 4 * block, hidden_width // 2 // TILES), BF16),
        pltpu.VMEM((TILES, 4 * block, hidden_width // 2 // TILES), F32),
        pltpu.SemaphoreType.DMA((6,)),
    ]
    return pl.pallas_call(
        functools.partial(step_kernel, size, plane, score_scale),
        out_shape=[
            jax.ShapeDtypeStruct((8, 128), F32),
            jax.ShapeDtypeStruct((chunk, across), F32),
        ],
        in_specs=[pl.BlockSpec(memory_space=pltpu.SMEM)] + [anywhere] * 2 + [vmem]
        + [anywhere] * 2,
        out_specs=[vmem] * 2,
        scratch_shapes=scratch,
        compiler_params=pltpu.CompilerParams(
            collective_id=0, has_side_effects=True, vmem_limit_bytes=60 * 1024 * 1024
        ),
    )(counts, *arrays)


def body(query_features, passage_features, counts, positives, w_first, w_second):
    device_count = lax.axis_size("dp")
    plane = 1 << device_count.bit_length() // 2
    score_scale = 2.5 * w_second.shape[1] ** (-0.5)
    loss, total = step(
        device_count,
        plane,
        score_scale,
        counts,
        query_features,
        passage_features,
        positives[None, :],
        w_first,
        w_second,
    )
    mean_loss, grad_first, grad_second = split_outputs(loss, total, w_first.shape[0])
    return (mean_loss[0], grad_first.T, grad_second)


def solution(mesh):
    return jax.shard_map(
        body,
        mesh=mesh,
        in_specs=(P("dp", None), P("dp", None), P(), P("dp"), P(), P()),
        out_specs=(P(), P(None, "dp"), P("dp", None)),
        check_vma=False,
    )
```

```python
import functools

import jax
import jax.numpy as jnp
from jax import lax
from jax.experimental import pallas as pl
from jax.experimental.pallas import tpu as pltpu
from jax.sharding import PartitionSpec as P

MESH = pl.DeviceIdType.MESH
F32 = jnp.float32
BF16 = jnp.bfloat16
GELU_ROOT = 0.7978845608028654
GELU_CUBE = 0.044715
TILES = 2
AHEAD = 3
DELAY = 2


def gelu_and_slope(value):
    square = value * value
    bent = jnp.tanh(GELU_ROOT * value * (1.0 + GELU_CUBE * square))
    rise = 0.5 * (1.0 + bent)
    slope = rise + 0.5 * value * (1.0 - bent * bent) * (
        GELU_ROOT * (1.0 + 3.0 * GELU_CUBE * square)
    )
    return value * rise, slope


def dot(left, right, left_dim, right_dim):
    return lax.dot_general(
        left, right, (((left_dim,), (right_dim,)), ((), ())), preferred_element_type=F32
    )


def flat_rows(blocks):
    return blocks.astype(F32).reshape(-1, blocks.shape[-1]).astype(BF16)


class Group:
    def __init__(self, send, recv):
        self.send, self.recv = send, recv

    def start(self, source, landing, device):
        pltpu.make_async_remote_copy(
            src_ref=source,
            dst_ref=landing,
            send_sem=self.send,
            recv_sem=self.recv,
            device_id=(device,),
            device_id_type=MESH,
        ).start()

    def landed(self, span):
        pltpu.make_async_copy(span, span, self.recv).wait()

    def sent(self, span):
        pltpu.make_async_copy(span, span, self.send).wait()

    def done(self, span):
        self.landed(span)
        self.sent(span)


class Groups:
    def __init__(self, send, recv):
        self.send, self.recv, self.used = send, recv, 0

    def new(self):
        self.used += 1
        assert self.used <= self.send.shape[0]
        return Group(self.send.at[self.used - 1], self.recv.at[self.used - 1])


def step_kernel(
    size,
    plane,
    score_scale,
    counts,
    query_hbm,
    passage_hbm,
    positives,
    w_first_hbm,
    w_second_hbm,
    out_loss,
    out_all,
    units_q,
    units_p,
    unit_mid_q,
    unit_mid_p,
    unit_pass,
    unit_land,
    unit_pos,
    feat_base,
    feat_tail,
    q_base,
    p_base,
    q_tail,
    q_extra,
    q_mid,
    q_unit,
    q_unit_land,
    p_tails,
    pos_land,
    all_q,
    all_p,
    scores,
    stat_land,
    found_land,
    dq_own_base,
    dq_own_tail,
    dq_pair_base,
    dq_pair_tail,
    dq_out_base,
    dq_out_tail,
    dq_land_base,
    dq_land_tail,
    dp_own_base,
    dp_own_tail,
    dp_out_base,
    dp_out_tail,
    dp_land_base,
    dp_land_tail,
    dp_relay_base,
    dp_relay_tail,
    loss_land,
    de_base,
    de_tail,
    all_x,
    own,
    outgoing,
    landing,
    outgoing_two,
    landing_two,
    sums,
    forward,
    landed,
    send_sems,
    recv_sems,
    line_send,
    line_recv,
    w_first,
    w_second,
    all_hidden,
    all_slope,
    load_sems,
):
    me = lax.axis_index("dp")
    rows = size // plane
    half = rows // 2
    lanes = plane // 2
    stride = size // 16
    row = lax.div(me, plane)
    spot = lax.rem(me, plane)
    core = lax.rem(me, 2)
    lane = lax.div(spot, 2)
    column = spot - core
    place = lax.div(me, stride)
    partner = me + 1 - 2 * core
    width, hidden_width = w_first.shape
    embed = w_second.shape[1]
    base = q_base.shape[1]
    unit = unit_pass.shape[1]
    hidden_half = hidden_width // 2
    tile = hidden_half // TILES
    per_tile = half // TILES
    chunk = hidden_half // (half * lanes * 2)
    groups = Groups(send_sems, recv_sems)

    plane_peers = [row * plane + lax.rem(spot + k, plane) for k in range(1, plane)]
    line_peers = [lax.rem(row + k, rows) * plane + spot for k in range(1, rows)]
    bits = [1 << at for at in range(lanes.bit_length() - 1)]
    lane_others = []
    for flips in range(1, lanes):
        away = lane
        for bit in bits:
            if flips & bit:
                away = away + bit - 2 * bit * lax.rem(lax.div(lane, bit), 2)
        lane_others.append(away)
    barrier = pltpu.get_barrier_semaphore()

    def greet(device):
        pl.semaphore_signal(barrier, inc=1, device_id=(device,), device_id_type=MESH)

    for k in range(1, 16):
        greet(lax.rem(place + k, 16) * stride + lax.rem(me, stride))
    for device in plane_peers:
        greet(device)
    in_column = 2 * row + core
    for k in range(1, 2 * rows):
        other = lax.rem(in_column + k, 2 * rows)
        greet(plane * lax.div(other, 2) + column + lax.rem(other, 2))

    spare = base + unit
    near = plane // stride
    aside = lax.div(spot, stride)
    for features, units, sem in ((passage_hbm, units_p, 1), (query_hbm, units_q, 0)):
        for u in range(15):
            there = u + lax.div(u + 16 - place, 16)
            pltpu.make_async_copy(
                features.at[pl.ds(spare + u * unit, unit), :],
                units.at[lax.div(there, near), lax.rem(there, near)],
                load_sems.at[sem],
            ).start()
        pltpu.make_async_copy(
            features.at[pl.ds(base, unit), :], units.at[row, aside], load_sems.at[sem]
        ).start()
    base_loads = [
        pltpu.make_async_copy(
            features.at[pl.ds(0, base), :], feat_base.at[core, at], load_sems.at[2 + at]
        )
        for at, features in enumerate((query_hbm, passage_hbm))
    ]
    weight_loads = [
        pltpu.make_async_copy(w_first_hbm, w_first, load_sems.at[4]),
        pltpu.make_async_copy(w_second_hbm, w_second, load_sems.at[5]),
    ]
    for load in base_loads + weight_loads:
        load.start()
    unit_pos[place] = positives[...].astype(F32)

    pl.semaphore_wait(barrier, 15 + plane - 1 + 2 * rows - 1)

    def units_loaded(features, sem):
        extra = features.at[pl.ds(base, 16 * unit), :]
        pltpu.make_async_copy(extra, extra, load_sems.at[sem]).wait()

    def spread_units(units, unit_mid):
        group = groups.new()
        for k in range(1, near):
            there = lax.rem(aside + k, near)
            group.start(
                units.at[:, there],
                unit_mid.at[aside],
                row * plane + there * stride + lax.rem(me, stride),
            )
        return group

    units_loaded(passage_hbm, 1)
    mid_p_group = spread_units(units_p, unit_mid_p)
    where_group = groups.new()
    for k in range(1, 16):
        device = lax.rem(place + k, 16) * stride + lax.rem(me, stride)
        where_group.start(unit_pos.at[place], unit_pos.at[place], device)

    heavies = []
    for g in range(stride):
        at = jnp.int32(0)
        for k in range(16):
            at = at + jnp.where(counts[g + stride * k] > base, g + stride * k, 0)
        heavies.append(at)
    source = jnp.int32(0)
    for g in range(stride):
        source = source + jnp.where(lax.rem(me, stride) == g, heavies[g], 0)

    def place_of(device):
        found_place = jnp.int32(0)
        for k in range(16):
            found_place = found_place + jnp.where(device >= stride * (k + 1), 1, 0)
        return found_place

    def row_and_aside(at):
        found_row, found_aside = jnp.int32(0), at
        for k in range(1, rows):
            beyond = at >= k * near
            found_row = found_row + jnp.where(beyond, 1, 0)
            found_aside = found_aside - jnp.where(beyond, near, 0)
        return found_row, found_aside

    heavy_place = place_of(source)
    source_row, source_aside = row_and_aside(heavy_place)

    def offset_of(device):
        before = jnp.int32(0)
        for at in heavies:
            before = before + jnp.where(at < device, 1, 0)
        return base * (device + before)

    def tail_row(device):
        piece = lax.div(device, stride) - jnp.where(source < device, 1, 0)
        return jnp.where(source == device, base, spare + unit * piece)

    def tower(features):
        total = None
        for low in range(0, hidden_width, tile):
            act = dot(features, w_first[:, low : low + tile], 1, 0)
            hidden = gelu_and_slope(act)[0].astype(BF16)
            part = dot(hidden, w_second[low : low + tile, :], 1, 0)
            total = part if total is None else total + part
        return total.astype(BF16)

    for load in base_loads:
        load.wait()
    pair_base = groups.new()
    pair_base.start(feat_base.at[core], feat_base.at[core], partner)
    for load in weight_loads:
        load.wait()
    units_loaded(query_hbm, 0)
    extra_x = flat_rows(units_q[...].reshape(16, unit, width))
    first_e = tower(jnp.concatenate([feat_base[core, 1], extra_x], axis=0))
    q_extra[...] = first_e[base:].astype(F32).reshape(q_extra.shape).astype(BF16)
    mid_e_group = spread_units(q_extra, q_mid)
    p_base[row] = first_e[:base]
    p_groups = [groups.new() for _ in range(rows)]
    relayed = rows == 4
    if relayed:

        def p_send(block, there, group):
            group.start(p_base.at[block], p_base.at[block], there * plane + spot)

        for at, order in enumerate(((2, 1), (3, 2, 0), (0, 1, 3), (1, 2))):

            @pl.when(row == at)
            def _():
                for there in order:
                    p_send(at, there, p_groups[at])
    else:
        for k in range(1, rows):
            p_groups[k].start(p_base.at[row], p_base.at[row], line_peers[k - 1])
    q_base[spot] = tower(feat_base[core, 0])
    q_pair = groups.new()
    q_pair.start(q_base.at[spot], q_base.at[spot], partner)
    q_groups = []
    for away in lane_others:
        group = groups.new()
        group.start(q_base.at[spot], q_base.at[spot], row * plane + 2 * away + core)
        q_groups.append(group)
    mid_q_group = spread_units(units_q, unit_mid_q)

    def picked(units, unit_mid):
        return jnp.where(
            source_aside == aside, units[:, aside].astype(F32), unit_mid[source_aside].astype(F32)
        )

    mid_e_group.done(q_mid.at[pl.ds(0, near - 1)])
    q_unit[...] = picked(q_extra, q_mid).astype(BF16)
    q_unit_group = groups.new()
    for k in range(1, rows):
        there = lax.rem(row + k, rows)
        q_unit_group.start(q_unit.at[there], q_unit_land.at[row], there * plane + spot)
    mid_p_group.done(unit_mid_p.at[pl.ds(0, near - 1)])
    passed = picked(units_p, unit_mid_p)
    unit_pass[:, :, width:] = passed.astype(BF16)
    tails = rows * unit
    p_tails[row] = tower(passed.reshape(tails, width).astype(BF16))
    p_tail_group, pass_group = groups.new(), groups.new()
    for device in line_peers:
        p_tail_group.start(p_tails.at[row], p_tails.at[row], device)

    where_group.done(unit_pos.at[pl.ds(0, 15)])
    slots = lax.broadcasted_iota(jnp.int32, (unit, positives.shape[1]), 1)
    chosen = lax.broadcasted_iota(jnp.int32, slots.shape, 0) + tail_row(me)
    tail_pos = jnp.sum(
        jnp.where(slots == chosen, unit_pos[heavy_place], 0.0), axis=1, keepdims=True
    )
    pos_land[spot, 0] = positives[:, :base].astype(F32)
    sub = lax.broadcasted_iota(jnp.int32, (unit, base), 0) + spot * unit
    along = lax.broadcasted_iota(jnp.int32, (unit, base), 1)
    pos_land[spot, 1] = jnp.sum(jnp.where(sub == along, tail_pos, 0.0), axis=0, keepdims=True)
    pos_group = groups.new()
    for device in plane_peers:
        pos_group.start(pos_land.at[spot], pos_land.at[spot], device)

    if relayed:
        for at, (far, end) in ((1, (3, 0)), (2, (0, 3))):

            @pl.when(row == at)
            def _():
                p_groups[far].landed(p_base.at[far])
                p_send(far, end, p_groups[far])

    def forward_q(at):
        there = 2 * lane_others[at] + core
        q_groups[at].done(q_base.at[there])
        q_pair.start(q_base.at[there], q_base.at[there], partner)

    for at in range(lanes - 1):
        forward_q(at)
    q_unit_group.done(q_unit_land.at[pl.ds(0, rows - 1)])
    q_tail[spot] = jnp.where(
        source_row == row, q_unit[row].astype(F32), q_unit_land[source_row].astype(F32)
    ).astype(BF16)
    q_tail_group = groups.new()
    for device in plane_peers:
        q_tail_group.start(q_tail.at[spot], q_tail.at[spot], device)
    if relayed:
        for at in range(rows):
            early = {0: 2, 3: 1}.get(at, at)

            @pl.when(jnp.logical_and(row != at, row != early))
            def _():
                p_groups[at].landed(p_base.at[at])
    else:
        for k in range(1, rows):
            p_groups[k].done(p_base.at[lax.rem(row + rows - k, rows)])
    q_pair.done(q_base.at[pl.ds(0, lanes)])

    q_rows, p_rows = plane * base, rows * base
    line = [plane * k + spot for k in range(rows)]
    base_ids = jnp.concatenate(
        [lax.broadcasted_iota(jnp.int32, (base, 1), 0) + offset_of(device) for device in line],
        axis=0,
    ).astype(F32)
    tail_ids = jnp.concatenate(
        [
            lax.broadcasted_iota(jnp.int32, (unit, 1), 0) + offset_of(source) + tail_row(device)
            for device in line
        ],
        axis=0,
    ).astype(F32)
    all_q[:q_rows] = q_base[...].reshape(q_rows, embed)
    all_p[:p_rows] = p_base[...].reshape(p_rows, embed)
    pos_group.done(pos_land.at[pl.ds(0, plane - 1)])
    base_wanted = jnp.concatenate([pos_land[k, 0] for k in range(plane)], axis=1)

    def spread(value, ids, wanted):
        top = jnp.max(value, axis=0, keepdims=True)
        mass = jnp.sum(jnp.exp(value - top), axis=0, keepdims=True)
        return top, mass, jnp.sum(jnp.where(ids == wanted, value, 0.0), axis=0, keepdims=True)

    def merge(one, two):
        top = jnp.maximum(one[0], two[0])
        mass = one[1] * jnp.exp(one[0] - top) + two[1] * jnp.exp(two[0] - top)
        return top, mass, one[2] + two[2]

    def scored(p_part, q_part):
        scores[p_part, q_part] = score_scale * dot(all_p[p_part], all_q[q_part], 1, 1)
        return scores[p_part, q_part]

    p_base_part, p_tail_part = slice(0, p_rows), slice(p_rows, all_p.shape[0])
    q_base_part, q_tail_part = slice(0, q_rows), slice(q_rows, all_q.shape[0])
    base_stats = spread(scored(p_base_part, q_base_part), base_ids, base_wanted)

    mid_q_group.done(unit_mid_q.at[pl.ds(0, near - 1)])
    unit_pass[:, :, :width] = picked(units_q, unit_mid_q).astype(BF16)
    for k in range(1, rows):
        there = lax.rem(row + k, rows)
        pass_group.start(unit_pass.at[there], unit_land.at[row], there * plane + spot)
    p_tail_group.done(p_tails.at[pl.ds(0, rows - 1)])
    all_p[p_rows:] = p_tails[source_row]
    base_stats = merge(
        base_stats, spread(scored(p_tail_part, q_base_part), tail_ids, base_wanted)
    )
    q_tail_group.done(q_tail.at[pl.ds(0, plane - 1)])
    all_q[q_rows:] = flat_rows(q_tail[...])
    pos_tail = pos_land[0, 1]
    for k in range(1, plane):
        pos_tail = pos_tail + pos_land[k, 1]
    tail_wanted = pos_tail[:, : plane * unit]
    ids = jnp.concatenate([base_ids, tail_ids], axis=0)
    tail_stats = spread(scored(slice(0, all_p.shape[0]), q_tail_part), ids, tail_wanted)
    stat_land[spot, 0:1, :q_rows] = base_stats[0]
    stat_land[spot, 0:1, q_rows:] = tail_stats[0]
    stat_land[spot, 1:2, :q_rows] = base_stats[1]
    stat_land[spot, 1:2, q_rows:] = tail_stats[1]
    found_land[spot, :, :q_rows] = base_stats[2]
    found_land[spot, :, q_rows:] = tail_stats[2]
    wanted = jnp.concatenate([base_wanted, tail_wanted], axis=1)
    hit = ids == wanted
    stat_group, found_group = groups.new(), groups.new()
    for device in plane_peers:
        stat_group.start(stat_land.at[spot], stat_land.at[spot], device)
    for device in plane_peers:
        found_group.start(found_land.at[spot], found_land.at[spot], device)
    pass_group.done(unit_land.at[pl.ds(0, rows - 1)])
    got = jnp.where(
        source_row == row, unit_pass[row].astype(F32), unit_land[source_row].astype(F32)
    )
    feat_tail[core, 0] = got[:, :width].astype(BF16)
    feat_tail[core, 1] = got[:, width:].astype(BF16)
    pair_tail = groups.new()
    pair_tail.start(feat_tail.at[core], feat_tail.at[core], partner)
    stat_group.done(stat_land.at[pl.ds(0, plane - 1)])
    stats = stat_land[...]
    tops = stats[:, 0]
    row_top = jnp.max(tops, axis=0, keepdims=True)
    mass = jnp.sum(stats[:, 1] * jnp.exp(tops - row_top), axis=0, keepdims=True)
    log_norm = row_top + jnp.log(mass)
    grads_t = (jnp.exp(scores[...] - log_norm) - hit.astype(F32)).astype(BF16)

    def hold(part, own_base, own_tail):
        rows_here = own_base.shape[0] * base
        own_base[...] = part[:rows_here].reshape(own_base.shape)
        own_tail[...] = part[rows_here:].reshape(own_tail.shape)

    dp_group, dp_tail_group, relay_group, relay_tail_group = [groups.new() for _ in range(4)]

    def send_dp(block, there, mine):
        device = there * plane + spot
        dp_group.start(dp_out_base.at[block], dp_land_base.at[mine], device)
        dp_tail_group.start(dp_out_tail.at[block], dp_land_tail.at[mine], device)

    hold(score_scale * dot(grads_t, all_q[...], 1, 0), dp_own_base, dp_own_tail)
    dp_out_base[...] = dp_own_base[...].astype(BF16)
    dp_out_tail[...] = dp_own_tail[...].astype(BF16)
    if relayed:
        for at, far, near_row, order in (
            (0, 3, 1, (2, 1)), (1, None, None, (2, 0)), (2, None, None, (1, 3)), (3, 0, 2, (1, 2))
        ):

            @pl.when(row == at)
            def _():
                if far is not None:
                    device = near_row * plane + spot
                    relay_group.start(dp_out_base.at[far], dp_relay_base, device)
                    relay_tail_group.start(dp_out_tail.at[far], dp_relay_tail, device)
                for there in order:
                    send_dp(there, there, at)
    else:
        for k in range(1, rows):
            there = lax.rem(row + k, rows)
            send_dp(there, there, row)

    hold(score_scale * dot(grads_t, all_p[...], 0, 0), dq_own_base, dq_own_tail)
    all_lanes = lane_others + [lane]
    pair_groups, pair_tail_group = [groups.new() for _ in all_lanes], groups.new()
    for there, group in zip(all_lanes, pair_groups):
        theirs = 2 * there + 1 - core
        group.start(dq_own_base.at[theirs], dq_pair_base.at[there], partner)
        pair_tail_group.start(dq_own_tail.at[theirs], dq_pair_tail.at[there], partner)
    found_group.done(found_land.at[pl.ds(0, plane - 1)])
    found = jnp.sum(found_land[...][:, 0], axis=0, keepdims=True)
    loss_land[row] = jnp.broadcast_to(
        jnp.sum(log_norm - found, axis=1, keepdims=True), loss_land.shape[1:]
    )
    loss_group = groups.new()
    for device in line_peers:
        loss_group.start(loss_land.at[row], loss_land.at[row], device)
    dq_group, dq_tail_group = groups.new(), groups.new()
    for there, group in zip(all_lanes, pair_groups):
        group.done(dq_pair_base.at[there])
        total = dq_own_base[2 * there + core] + dq_pair_base[there]
        if there is lane:
            dq_mine = total
        else:
            dq_out_base[there] = total.astype(BF16)
            device = row * plane + 2 * there + core
            dq_group.start(dq_out_base.at[there], dq_land_base.at[lane], device)
    pair_tail_group.done(dq_pair_tail.at[pl.ds(0, lanes)])
    for there in lane_others:
        dq_out_tail[there] = (dq_own_tail[2 * there + core] + dq_pair_tail[there]).astype(BF16)
        device = row * plane + 2 * there + core
        dq_tail_group.start(dq_out_tail.at[there], dq_land_tail.at[lane], device)
    dq_mine_tail = dq_own_tail[2 * lane + core] + dq_pair_tail[lane]
    if relayed:
        for at, far in ((1, 3), (2, 0)):

            @pl.when(row == at)
            def _():
                relay_group.landed(dp_relay_base)
                relay_tail_group.landed(dp_relay_tail)
                dp_out_base[far] = (dp_own_base[far] + dp_relay_base[...].astype(F32)).astype(BF16)
                dp_out_tail[far] = (dp_own_tail[far] + dp_relay_tail[...].astype(F32)).astype(BF16)
                send_dp(far, far, at)

    pair_base.done(feat_base.at[0])
    pair_tail.done(feat_tail.at[0])
    x_rows = 4 * base
    all_x[:x_rows] = feat_base[...].reshape(x_rows, width)
    all_x[x_rows:] = flat_rows(feat_tail[...])
    for t in range(TILES):
        start = pl.multiple_of(core * hidden_half + t * tile, 128)
        hidden, slope = gelu_and_slope(dot(all_x[...], w_first[:, pl.ds(start, tile)], 1, 0))
        all_hidden[t] = hidden.astype(BF16)
        all_slope[t] = slope
    dq_group.done(dq_land_base.at[pl.ds(0, lanes - 1)])
    dq_tail_group.done(dq_land_tail.at[pl.ds(0, lanes - 1)])
    for there in lane_others:
        dq_mine = dq_mine + dq_land_base[there].astype(F32)
        dq_mine_tail = dq_mine_tail + dq_land_tail[there].astype(F32)
    de_base[core, 0] = dq_mine.astype(BF16)
    de_tail[core, 0] = dq_mine_tail.astype(BF16)

    def send_de(side):
        base_group, tail_group = groups.new(), groups.new()
        base_group.start(de_base.at[core, side], de_base.at[core, side], partner)
        tail_group.start(de_tail.at[core, side], de_tail.at[core, side], partner)

        def finish():
            base_group.done(de_base.at[0, side])
            tail_group.done(de_tail.at[0, side])

        return finish

    finish_pair = [send_de(0)]
    def dp_landed(count):
        dp_group.done(dp_land_base.at[pl.ds(0, count)])
        dp_tail_group.done(dp_land_tail.at[pl.ds(0, count)])

    if relayed:
        ends = lax.rem(row, 3) == 0

        @pl.when(ends)
        def _():
            dp_landed(2)
            relay_group.sent(dp_relay_base)
            relay_tail_group.sent(dp_relay_tail)

        @pl.when(jnp.logical_not(ends))
        def _():
            dp_landed(3)
    else:
        dp_landed(rows - 1)
    dp_mine, dp_mine_tail = dp_own_base[row], dp_own_tail[row]
    for k in range(1, rows):
        there = lax.rem(row + k, rows)
        part, part_tail = dp_land_base[there].astype(F32), dp_land_tail[there].astype(F32)
        if relayed:
            used = jnp.logical_not(jnp.logical_and(ends, row + there == 3))
            part, part_tail = jnp.where(used, part, 0.0), jnp.where(used, part_tail, 0.0)
        dp_mine, dp_mine_tail = dp_mine + part, dp_mine_tail + part_tail
    de_base[core, 1] = dp_mine.astype(BF16)
    de_tail[core, 1] = dp_mine_tail.astype(BF16)
    finish_pair.append(send_de(1))
    low_count, high_count = 2, lanes // 2
    low_lane, high_lane = lax.rem(lane, low_count), lax.div(lane, low_count)
    low_others = [lax.rem(low_lane + k, low_count) for k in range(1, low_count)]
    high_others = [lax.rem(high_lane + k, high_count) for k in range(1, high_count)]
    skip, skip_two = half * lanes, half * high_count

    def in_plane(high, low):
        return plane * row + 2 * (high * low_count + low) + core

    def first_stage(chunk_at, part):
        t, cols = chunk_at
        for i in range(per_tile):
            for high in range(high_count):
                for low in range(low_count):
                    for j in range(2):
                        at = (((i * high_count + high) * low_count + low) * 2 + j) * chunk
                        piece = part[at : at + chunk]
                        step = t * per_tile + i
                        own[step, j, high, low, :, cols] = piece
                        if j == 0:
                            slot = (low * half + step) * high_count + high
                        else:
                            slot = skip + (high * half + step) * low_count + low
                        outgoing[slot, :, cols] = piece.astype(BF16)
        group = groups.new()
        span = per_tile * high_count
        for low in low_others:
            group.start(
                outgoing.at[pl.ds((low * half + t * per_tile) * high_count, span), :, cols],
                landing.at[pl.ds((low_lane * half + t * per_tile) * high_count, span), :, cols],
                in_plane(high_lane, low),
            )
        span = per_tile * low_count
        for high in high_others:
            group.start(
                outgoing.at[pl.ds(skip + (high * half + t * per_tile) * low_count, span), :, cols],
                landing.at[pl.ds(skip + (high_lane * half + t * per_tile) * low_count, span), :, cols],
                in_plane(high, low_lane),
            )
        return group

    def second_stage(chunk_at, before):
        t, cols = chunk_at
        count = (low_count - 1) * high_count + (high_count - 1) * low_count
        before.done(landing.at[pl.ds(0, per_tile * count), :, cols])
        for i in range(t * per_tile, (t + 1) * per_tile):
            for high in range(high_count):
                total = own[i, 0, high, low_lane, :, cols]
                for low in low_others:
                    total = total + landing[(low * half + i) * high_count + high, :, cols].astype(F32)
                own[i, 0, high, low_lane, :, cols] = total
                outgoing_two[high * half + i, :, cols] = total.astype(BF16)
            for low in range(low_count):
                total = own[i, 1, high_lane, low, :, cols]
                for high in high_others:
                    slot = skip + (high * half + i) * low_count + low
                    total = total + landing[slot, :, cols].astype(F32)
                own[i, 1, high_lane, low, :, cols] = total
                outgoing_two[skip_two + low * half + i, :, cols] = total.astype(BF16)
        group = groups.new()
        block = t * per_tile
        for high in high_others:
            group.start(
                outgoing_two.at[pl.ds(high * half + block, per_tile), :, cols],
                landing_two.at[pl.ds(high_lane * half + block, per_tile), :, cols],
                in_plane(high, low_lane),
            )
        for low in low_others:
            group.start(
                outgoing_two.at[pl.ds(skip_two + low * half + block, per_tile), :, cols],
                landing_two.at[pl.ds(skip_two + low_lane * half + block, per_tile), :, cols],
                in_plane(high_lane, low),
            )
        return group

    def line_copy(i, j, cols):
        return pltpu.make_async_remote_copy(
            src_ref=forward.at[i, j, :, cols],
            dst_ref=landed.at[row, :, cols],
            send_sem=line_send.at[i, j],
            recv_sem=line_recv.at[row],
            device_id=(plane * (half * core + i) + column + j,),
            device_id_type=MESH,
        )

    def third_stage(chunk_at, before):
        t, cols = chunk_at
        count = low_count - 1 + high_count - 1
        before.done(landing_two.at[pl.ds(0, per_tile * count), :, cols])
        for i in range(t * per_tile, (t + 1) * per_tile):
            for j in range(2):
                total = own[i, j, high_lane, low_lane, :, cols]
                if j == 0:
                    slots = [high * half + i for high in high_others]
                else:
                    slots = [skip_two + low * half + i for low in low_others]
                for slot in slots:
                    total = total + landing_two[slot, :, cols].astype(F32)
                sums[i, j, :, cols] = total
                forward[i, j, :, cols] = total.astype(BF16)

                @pl.when(plane * (half * core + i) + column + j != me)
                def _():
                    line_copy(i, j, cols).start()

    for finish in finish_pair:
        finish()
    de = jnp.concatenate([de_base[...].reshape(x_rows, embed), flat_rows(de_tail[...])], axis=0)
    act_grads = {}

    def part_of(chunk_at):
        t, cols = chunk_at
        if cols.start >= width:
            return dot(all_hidden[t], de[:, cols.start - width : cols.start - width + cols.size], 0, 0)
        if t not in act_grads:
            start = pl.multiple_of(core * hidden_half + t * tile, 128)
            back = dot(de, w_second[pl.ds(start, tile), :], 1, 1)
            act_grads[t] = (all_slope[t] * back).astype(BF16)
        return dot(act_grads[t], all_x[:, cols], 0, 0)

    piece = embed
    chunks = []
    for t in range(TILES):
        chunks.append((t, pl.ds(width, piece)))
        for low in range(0, width, piece):
            chunks.append((t, pl.ds(low, piece)))
    ones, twos = [], []
    for at in range(len(chunks) + DELAY):
        if at < len(chunks):
            for ahead in range(len(ones), min(at + AHEAD, len(chunks))):
                ones.append(first_stage(chunks[ahead], part_of(chunks[ahead])))
            twos.append(second_stage(chunks[at], ones[at]))
        if at >= DELAY:
            third_stage(chunks[at - DELAY], twos[at - DELAY])

    if relayed:
        for at in range(rows):

            @pl.when(row == at)
            def _():
                p_groups[at].sent(p_base.at[pl.ds(0, 3 if at in (1, 2) else 2)])
                if at in (1, 2):
                    far = 3 if at == 1 else 0
                    p_groups[far].sent(p_base.at[far])

    sender_core = lax.div(row, half)
    whole = pl.ds(0, width + embed)
    for i in range(half):
        for j in range(2):

            @pl.when(plane * (half * core + i) + column + j != me)
            def _():
                line_copy(i, j, whole).wait_send()

    for sender_row in range(rows):
        sender = plane * sender_row + column + sender_core

        @pl.when(sender != me)
        def _():
            pltpu.make_async_remote_copy(
                src_ref=forward.at[0, 0],
                dst_ref=landed.at[sender_row],
                send_sem=line_send.at[0, 0],
                recv_sem=line_recv.at[sender_row],
                device_id=(sender,),
                device_id_type=MESH,
            ).wait_recv()

    total = jnp.where(sender_core == core, sums[lax.rem(row, half), core], 0.0)
    for sender_row in range(rows):
        sender = plane * sender_row + column + sender_core
        total = total + jnp.where(sender == me, 0.0, landed[sender_row].astype(F32))
    out_all[...] = total
    loss_group.done(loss_land.at[pl.ds(0, rows - 1)])
    loss = loss_land[0]
    for k in range(1, rows):
        loss = loss + loss_land[k]
    out_loss[...] = loss * (1.0 / (size * spare))


def split_kernel(loss, total, mean_loss, first, second):
    width = first.shape[1]
    mean_loss[0] = loss[0, 0]
    first[...] = total[:, :width]
    second[...] = total[:, width:]


def split_outputs(loss, total, width):
    vmem = pl.BlockSpec(memory_space=pltpu.VMEM)
    chunk, across = total.shape
    return pl.pallas_call(
        split_kernel,
        out_shape=[
            jax.ShapeDtypeStruct((1,), F32),
            jax.ShapeDtypeStruct((chunk, width), F32),
            jax.ShapeDtypeStruct((chunk, across - width), F32),
        ],
        in_specs=[pl.BlockSpec(memory_space=pltpu.SMEM), vmem],
        out_specs=[pl.BlockSpec(memory_space=pltpu.SMEM), vmem, vmem],
    )(loss, total)


def step(size, plane, score_scale, counts, *arrays):
    query_features, _, positives, w_first, w_second = arrays
    rows, lanes = size // plane, plane // 2
    half = rows // 2
    width, hidden_width = w_first.shape
    embed = w_second.shape[1]
    chunk = hidden_width // size
    across = width + embed
    base = query_features.shape[0] // 2
    unit = base // 16
    block = base + unit
    vmem = pl.BlockSpec(memory_space=pltpu.VMEM)
    anywhere = pl.BlockSpec(memory_space=pl.ANY)
    count = 26 + rows + 2 * lanes + 2 * TILES * (1 + width // embed)

    def split(members, dtype):
        return [
            pltpu.VMEM((members, base, embed), dtype),
            pltpu.VMEM((members, unit, embed), dtype),
        ]

    scratch = [
        pltpu.VMEM((rows, 16 // rows, unit, width), BF16),
        pltpu.VMEM((rows, 16 // rows, unit, width), BF16),
        pltpu.VMEM((16 // rows, rows, unit, width), BF16),
        pltpu.VMEM((16 // rows, rows, unit, width), BF16),
        pltpu.VMEM((rows, unit, 2 * width), BF16),
        pltpu.VMEM((rows, unit, 2 * width), BF16),
        pltpu.VMEM((16,) + positives.shape, F32),
        pltpu.VMEM((2, 2, base, width), BF16),
        pltpu.VMEM((2, 2, unit, width), BF16),
        pltpu.VMEM((plane, base, embed), BF16),
        pltpu.VMEM((rows, base, embed), BF16),
        pltpu.VMEM((plane, unit, embed), BF16),
        pltpu.VMEM((rows, 16 // rows, unit, embed), BF16),
        pltpu.VMEM((16 // rows, rows, unit, embed), BF16),
        pltpu.VMEM((rows, unit, embed), BF16),
        pltpu.VMEM((rows, unit, embed), BF16),
        pltpu.VMEM((rows, rows * unit, embed), BF16),
        pltpu.VMEM((plane, 2, 1, base), F32),
        pltpu.VMEM((plane * block, embed), BF16),
        pltpu.VMEM((rows * block, embed), BF16),
        pltpu.VMEM((rows * block, plane * block), F32),
        pltpu.VMEM((plane, 2, plane * block), F32),
        pltpu.VMEM((plane, 1, plane * block), F32),
        *split(plane, F32),
        *split(lanes, F32),
        *split(lanes, BF16),
        *split(lanes, BF16),
        *split(rows, F32),
        *split(rows, BF16),
        *split(rows, BF16),
        pltpu.VMEM((base, embed), BF16),
        pltpu.VMEM((unit, embed), BF16),
        pltpu.VMEM((rows, 8, 128), F32),
        pltpu.VMEM((2, 2, base, embed), BF16),
        pltpu.VMEM((2, 2, unit, embed), BF16),
        pltpu.VMEM((4 * block, width), BF16),
        pltpu.VMEM((half, 2, lanes // 2, 2, chunk, across), F32),
        pltpu.VMEM((2 * half * lanes, chunk, across), BF16),
        pltpu.VMEM((2 * half * lanes, chunk, across), BF16),
        pltpu.VMEM((half * (lanes // 2 + 2), chunk, across), BF16),
        pltpu.VMEM((half * (lanes // 2 + 2), chunk, across), BF16),
        pltpu.VMEM((half, 2, chunk, across), F32),
        pltpu.VMEM((half, 2, chunk, across), BF16),
        pltpu.VMEM((rows, chunk, across), BF16),
        pltpu.SemaphoreType.DMA((count,)),
        pltpu.SemaphoreType.DMA((count,)),
        pltpu.SemaphoreType.DMA((half, 2)),
        pltpu.SemaphoreType.DMA((rows,)),
        pltpu.VMEM(w_first.shape, BF16),
        pltpu.VMEM(w_second.shape, BF16),
        pltpu.VMEM((TILES, 4 * block, hidden_width // 2 // TILES), BF16),
        pltpu.VMEM((TILES, 4 * block, hidden_width // 2 // TILES), F32),
        pltpu.SemaphoreType.DMA((6,)),
    ]
    return pl.pallas_call(
        functools.partial(step_kernel, size, plane, score_scale),
        out_shape=[
            jax.ShapeDtypeStruct((8, 128), F32),
            jax.ShapeDtypeStruct((chunk, across), F32),
        ],
        in_specs=[pl.BlockSpec(memory_space=pltpu.SMEM)] + [anywhere] * 2 + [vmem]
        + [anywhere] * 2,
        out_specs=[vmem] * 2,
        scratch_shapes=scratch,
        compiler_params=pltpu.CompilerParams(
            collective_id=0, has_side_effects=True, vmem_limit_bytes=60 * 1024 * 1024
        ),
    )(counts, *arrays)


def body(query_features, passage_features, counts, positives, w_first, w_second):
    device_count = lax.axis_size("dp")
    plane = 1 << device_count.bit_length() // 2
    score_scale = 2.5 * w_second.shape[1] ** (-0.5)
    loss, total = step(
        device_count,
        plane,
        score_scale,
        counts,
        query_features,
        passage_features,
        positives[None, :],
        w_first,
        w_second,
    )
    mean_loss, grad_first, grad_second = split_outputs(loss, total, w_first.shape[0])
    return (mean_loss[0], grad_first.T, grad_second)


def solution(mesh):
    return jax.shard_map(
        body,
        mesh=mesh,
        in_specs=(P("dp", None), P("dp", None), P(), P("dp"), P(), P()),
        out_specs=(P(), P(None, "dp"), P("dp", None)),
        check_vma=False,
    )
```

```python
import functools

import jax
import jax.numpy as jnp
from jax import lax
from jax.experimental import pallas as pl
from jax.experimental.pallas import tpu as pltpu
from jax.sharding import PartitionSpec as P

MESH = pl.DeviceIdType.MESH
F32 = jnp.float32
BF16 = jnp.bfloat16
GELU_ROOT = 0.7978845608028654
GELU_CUBE = 0.044715
TILES = 2
AHEAD = 3
DELAY = 2
LAST = 128
BEHIND = 0


def gelu_and_slope(value):
    square = value * value
    bent = jnp.tanh(GELU_ROOT * value * (1.0 + GELU_CUBE * square))
    rise = 0.5 * (1.0 + bent)
    slope = rise + 0.5 * value * (1.0 - bent * bent) * (
        GELU_ROOT * (1.0 + 3.0 * GELU_CUBE * square)
    )
    return value * rise, slope


def dot(left, right, left_dim, right_dim):
    return lax.dot_general(
        left, right, (((left_dim,), (right_dim,)), ((), ())), preferred_element_type=F32
    )


def flat_rows(blocks):
    return blocks.astype(F32).reshape(-1, blocks.shape[-1]).astype(BF16)


class Group:
    def __init__(self, send, recv):
        self.send, self.recv = send, recv

    def start(self, source, landing, device):
        pltpu.make_async_remote_copy(
            src_ref=source,
            dst_ref=landing,
            send_sem=self.send,
            recv_sem=self.recv,
            device_id=(device,),
            device_id_type=MESH,
        ).start()

    def landed(self, span):
        pltpu.make_async_copy(span, span, self.recv).wait()

    def sent(self, span):
        pltpu.make_async_copy(span, span, self.send).wait()

    def done(self, span):
        self.landed(span)
        self.sent(span)


class Groups:
    def __init__(self, send, recv):
        self.send, self.recv, self.used = send, recv, 0

    def new(self):
        self.used += 1
        assert self.used <= self.send.shape[0]
        return Group(self.send.at[self.used - 1], self.recv.at[self.used - 1])


def step_kernel(
    size,
    plane,
    score_scale,
    counts,
    query_hbm,
    passage_hbm,
    positives,
    w_first_hbm,
    w_second_hbm,
    out_loss,
    out_all,
    units_q,
    units_p,
    unit_mid_q,
    unit_mid_p,
    unit_pass,
    unit_land,
    unit_pos,
    feat_base,
    feat_tail,
    q_base,
    p_base,
    q_tail,
    q_extra,
    q_mid,
    q_unit,
    q_unit_land,
    p_tails,
    pos_land,
    all_q,
    all_p,
    scores,
    stat_land,
    found_land,
    dq_own_base,
    dq_own_tail,
    dq_pair_base,
    dq_pair_tail,
    dq_out_base,
    dq_out_tail,
    dq_land_base,
    dq_land_tail,
    dp_own_base,
    dp_own_tail,
    dp_out_base,
    dp_out_tail,
    dp_land_base,
    dp_land_tail,
    dp_relay_base,
    dp_relay_tail,
    loss_land,
    de_base,
    de_tail,
    all_x,
    own,
    outgoing,
    landing,
    outgoing_two,
    landing_two,
    landing_direct,
    sums,
    forward,
    landed,
    send_sems,
    recv_sems,
    line_send,
    line_recv,
    w_first,
    w_second,
    all_hidden,
    all_slope,
    load_sems,
):
    me = lax.axis_index("dp")
    rows = size // plane
    half = rows // 2
    lanes = plane // 2
    stride = size // 16
    row = lax.div(me, plane)
    spot = lax.rem(me, plane)
    core = lax.rem(me, 2)
    lane = lax.div(spot, 2)
    column = spot - core
    place = lax.div(me, stride)
    partner = me + 1 - 2 * core
    width, hidden_width = w_first.shape
    embed = w_second.shape[1]
    base = q_base.shape[1]
    unit = unit_pass.shape[1]
    hidden_half = hidden_width // 2
    tile = hidden_half // TILES
    per_tile = half // TILES
    chunk = hidden_half // (half * lanes * 2)
    groups = Groups(send_sems, recv_sems)

    plane_peers = [row * plane + lax.rem(spot + k, plane) for k in range(1, plane)]
    line_peers = [lax.rem(row + k, rows) * plane + spot for k in range(1, rows)]
    bits = [1 << at for at in range(lanes.bit_length() - 1)]
    lane_others = []
    for flips in range(1, lanes):
        away = lane
        for bit in bits:
            if flips & bit:
                away = away + bit - 2 * bit * lax.rem(lax.div(lane, bit), 2)
        lane_others.append(away)
    barrier = pltpu.get_barrier_semaphore()

    def greet(device):
        pl.semaphore_signal(barrier, inc=1, device_id=(device,), device_id_type=MESH)

    for k in range(1, 16):
        greet(lax.rem(place + k, 16) * stride + lax.rem(me, stride))
    for device in plane_peers:
        greet(device)
    in_column = 2 * row + core
    for k in range(1, 2 * rows):
        other = lax.rem(in_column + k, 2 * rows)
        greet(plane * lax.div(other, 2) + column + lax.rem(other, 2))

    spare = base + unit
    near = plane // stride
    aside = lax.div(spot, stride)
    for features, units, sem in ((passage_hbm, units_p, 1), (query_hbm, units_q, 0)):
        for u in range(15):
            there = u + lax.div(u + 16 - place, 16)
            pltpu.make_async_copy(
                features.at[pl.ds(spare + u * unit, unit), :],
                units.at[lax.div(there, near), lax.rem(there, near)],
                load_sems.at[sem],
            ).start()
        pltpu.make_async_copy(
            features.at[pl.ds(base, unit), :], units.at[row, aside], load_sems.at[sem]
        ).start()
    base_loads = [
        pltpu.make_async_copy(
            features.at[pl.ds(0, base), :], feat_base.at[core, at], load_sems.at[2 + at]
        )
        for at, features in enumerate((query_hbm, passage_hbm))
    ]
    weight_loads = [
        pltpu.make_async_copy(w_first_hbm, w_first, load_sems.at[4]),
        pltpu.make_async_copy(w_second_hbm, w_second, load_sems.at[5]),
    ]
    for load in base_loads + weight_loads:
        load.start()
    unit_pos[place] = positives[...].astype(F32)

    pl.semaphore_wait(barrier, 15 + plane - 1 + 2 * rows - 1)

    def units_loaded(features, sem):
        extra = features.at[pl.ds(base, 16 * unit), :]
        pltpu.make_async_copy(extra, extra, load_sems.at[sem]).wait()

    def spread_units(units, unit_mid):
        group = groups.new()
        for k in range(1, near):
            there = lax.rem(aside + k, near)
            group.start(
                units.at[:, there],
                unit_mid.at[aside],
                row * plane + there * stride + lax.rem(me, stride),
            )
        return group

    units_loaded(passage_hbm, 1)
    mid_p_group = spread_units(units_p, unit_mid_p)
    where_group = groups.new()
    for k in range(1, 16):
        device = lax.rem(place + k, 16) * stride + lax.rem(me, stride)
        where_group.start(unit_pos.at[place], unit_pos.at[place], device)

    heavies = []
    for g in range(stride):
        at = jnp.int32(0)
        for k in range(16):
            at = at + jnp.where(counts[g + stride * k] > base, g + stride * k, 0)
        heavies.append(at)
    source = jnp.int32(0)
    for g in range(stride):
        source = source + jnp.where(lax.rem(me, stride) == g, heavies[g], 0)

    def place_of(device):
        found_place = jnp.int32(0)
        for k in range(16):
            found_place = found_place + jnp.where(device >= stride * (k + 1), 1, 0)
        return found_place

    def row_and_aside(at):
        found_row, found_aside = jnp.int32(0), at
        for k in range(1, rows):
            beyond = at >= k * near
            found_row = found_row + jnp.where(beyond, 1, 0)
            found_aside = found_aside - jnp.where(beyond, near, 0)
        return found_row, found_aside

    heavy_place = place_of(source)
    source_row, source_aside = row_and_aside(heavy_place)

    def offset_of(device):
        before = jnp.int32(0)
        for at in heavies:
            before = before + jnp.where(at < device, 1, 0)
        return base * (device + before)

    def tail_row(device):
        piece = lax.div(device, stride) - jnp.where(source < device, 1, 0)
        return jnp.where(source == device, base, spare + unit * piece)

    def tower(features):
        total = None
        for low in range(0, hidden_width, tile):
            act = dot(features, w_first[:, low : low + tile], 1, 0)
            hidden = gelu_and_slope(act)[0].astype(BF16)
            part = dot(hidden, w_second[low : low + tile, :], 1, 0)
            total = part if total is None else total + part
        return total.astype(BF16)

    for load in base_loads:
        load.wait()
    pair_base = groups.new()
    pair_base.start(feat_base.at[core], feat_base.at[core], partner)
    for load in weight_loads:
        load.wait()
    units_loaded(query_hbm, 0)
    extra_x = flat_rows(units_q[...].reshape(16, unit, width))
    first_e = tower(jnp.concatenate([feat_base[core, 1], extra_x], axis=0))
    q_extra[...] = first_e[base:].astype(F32).reshape(q_extra.shape).astype(BF16)
    mid_e_group = spread_units(q_extra, q_mid)
    p_base[row] = first_e[:base]
    p_groups = [groups.new() for _ in range(rows)]
    relayed = rows == 4
    if relayed:

        def p_send(block, there, group):
            group.start(p_base.at[block], p_base.at[block], there * plane + spot)

        for at, order in enumerate(((2, 1), (3, 2, 0), (0, 1, 3), (1, 2))):

            @pl.when(row == at)
            def _():
                for there in order:
                    p_send(at, there, p_groups[at])
    else:
        for k in range(1, rows):
            p_groups[k].start(p_base.at[row], p_base.at[row], line_peers[k - 1])
    q_base[spot] = tower(feat_base[core, 0])
    q_pair = groups.new()
    q_pair.start(q_base.at[spot], q_base.at[spot], partner)
    q_groups = []
    for away in lane_others:
        group = groups.new()
        group.start(q_base.at[spot], q_base.at[spot], row * plane + 2 * away + core)
        q_groups.append(group)
    mid_q_group = spread_units(units_q, unit_mid_q)

    def picked(units, unit_mid):
        return jnp.where(
            source_aside == aside, units[:, aside].astype(F32), unit_mid[source_aside].astype(F32)
        )

    mid_e_group.done(q_mid.at[pl.ds(0, near - 1)])
    q_unit[...] = picked(q_extra, q_mid).astype(BF16)
    q_unit_group = groups.new()
    for k in range(1, rows):
        there = lax.rem(row + k, rows)
        q_unit_group.start(q_unit.at[there], q_unit_land.at[row], there * plane + spot)
    mid_p_group.done(unit_mid_p.at[pl.ds(0, near - 1)])
    passed = picked(units_p, unit_mid_p)
    unit_pass[:, :, width:] = passed.astype(BF16)
    tails = rows * unit
    p_tails[row] = tower(passed.reshape(tails, width).astype(BF16))
    p_tail_group, pass_group = groups.new(), groups.new()
    for device in line_peers:
        p_tail_group.start(p_tails.at[row], p_tails.at[row], device)

    where_group.done(unit_pos.at[pl.ds(0, 15)])
    slots = lax.broadcasted_iota(jnp.int32, (unit, positives.shape[1]), 1)
    chosen = lax.broadcasted_iota(jnp.int32, slots.shape, 0) + tail_row(me)
    tail_pos = jnp.sum(
        jnp.where(slots == chosen, unit_pos[heavy_place], 0.0), axis=1, keepdims=True
    )
    pos_land[spot, 0] = positives[:, :base].astype(F32)
    sub = lax.broadcasted_iota(jnp.int32, (unit, base), 0) + spot * unit
    along = lax.broadcasted_iota(jnp.int32, (unit, base), 1)
    pos_land[spot, 1] = jnp.sum(jnp.where(sub == along, tail_pos, 0.0), axis=0, keepdims=True)
    pos_group = groups.new()
    for device in plane_peers:
        pos_group.start(pos_land.at[spot], pos_land.at[spot], device)

    if relayed:
        for at, (far, end) in ((1, (3, 0)), (2, (0, 3))):

            @pl.when(row == at)
            def _():
                p_groups[far].landed(p_base.at[far])
                p_send(far, end, p_groups[far])

    def forward_q(at):
        there = 2 * lane_others[at] + core
        q_groups[at].done(q_base.at[there])
        q_pair.start(q_base.at[there], q_base.at[there], partner)

    for at in range(lanes - 1):
        forward_q(at)
    q_unit_group.done(q_unit_land.at[pl.ds(0, rows - 1)])
    q_tail[spot] = jnp.where(
        source_row == row, q_unit[row].astype(F32), q_unit_land[source_row].astype(F32)
    ).astype(BF16)
    q_tail_group = groups.new()
    for device in plane_peers:
        q_tail_group.start(q_tail.at[spot], q_tail.at[spot], device)
    if relayed:
        for at in range(rows):
            early = {0: 2, 3: 1}.get(at, at)

            @pl.when(jnp.logical_and(row != at, row != early))
            def _():
                p_groups[at].landed(p_base.at[at])
    else:
        for k in range(1, rows):
            p_groups[k].done(p_base.at[lax.rem(row + rows - k, rows)])
    q_pair.done(q_base.at[pl.ds(0, lanes)])

    q_rows, p_rows = plane * base, rows * base
    line = [plane * k + spot for k in range(rows)]
    base_ids = jnp.concatenate(
        [lax.broadcasted_iota(jnp.int32, (base, 1), 0) + offset_of(device) for device in line],
        axis=0,
    ).astype(F32)
    tail_ids = jnp.concatenate(
        [
            lax.broadcasted_iota(jnp.int32, (unit, 1), 0) + offset_of(source) + tail_row(device)
            for device in line
        ],
        axis=0,
    ).astype(F32)
    all_q[:q_rows] = q_base[...].reshape(q_rows, embed)
    all_p[:p_rows] = p_base[...].reshape(p_rows, embed)
    pos_group.done(pos_land.at[pl.ds(0, plane - 1)])
    base_wanted = jnp.concatenate([pos_land[k, 0] for k in range(plane)], axis=1)

    def spread(value, ids, wanted):
        top = jnp.max(value, axis=0, keepdims=True)
        mass = jnp.sum(jnp.exp(value - top), axis=0, keepdims=True)
        return top, mass, jnp.sum(jnp.where(ids == wanted, value, 0.0), axis=0, keepdims=True)

    def merge(one, two):
        top = jnp.maximum(one[0], two[0])
        mass = one[1] * jnp.exp(one[0] - top) + two[1] * jnp.exp(two[0] - top)
        return top, mass, one[2] + two[2]

    def scored(p_part, q_part):
        scores[p_part, q_part] = score_scale * dot(all_p[p_part], all_q[q_part], 1, 1)
        return scores[p_part, q_part]

    p_base_part, p_tail_part = slice(0, p_rows), slice(p_rows, all_p.shape[0])
    q_base_part, q_tail_part = slice(0, q_rows), slice(q_rows, all_q.shape[0])
    base_stats = spread(scored(p_base_part, q_base_part), base_ids, base_wanted)

    mid_q_group.done(unit_mid_q.at[pl.ds(0, near - 1)])
    unit_pass[:, :, :width] = picked(units_q, unit_mid_q).astype(BF16)
    for k in range(1, rows):
        there = lax.rem(row + k, rows)
        pass_group.start(unit_pass.at[there], unit_land.at[row], there * plane + spot)
    p_tail_group.done(p_tails.at[pl.ds(0, rows - 1)])
    all_p[p_rows:] = p_tails[source_row]
    base_stats = merge(
        base_stats, spread(scored(p_tail_part, q_base_part), tail_ids, base_wanted)
    )
    q_tail_group.done(q_tail.at[pl.ds(0, plane - 1)])
    all_q[q_rows:] = flat_rows(q_tail[...])
    pos_tail = pos_land[0, 1]
    for k in range(1, plane):
        pos_tail = pos_tail + pos_land[k, 1]
    tail_wanted = pos_tail[:, : plane * unit]
    ids = jnp.concatenate([base_ids, tail_ids], axis=0)
    tail_stats = spread(scored(slice(0, all_p.shape[0]), q_tail_part), ids, tail_wanted)
    stat_land[spot, 0:1, :q_rows] = base_stats[0]
    stat_land[spot, 0:1, q_rows:] = tail_stats[0]
    stat_land[spot, 1:2, :q_rows] = base_stats[1]
    stat_land[spot, 1:2, q_rows:] = tail_stats[1]
    found_land[spot, :, :q_rows] = base_stats[2]
    found_land[spot, :, q_rows:] = tail_stats[2]
    wanted = jnp.concatenate([base_wanted, tail_wanted], axis=1)
    hit = ids == wanted
    stat_group, found_group = groups.new(), groups.new()
    for device in plane_peers:
        stat_group.start(stat_land.at[spot], stat_land.at[spot], device)
    for device in plane_peers:
        found_group.start(found_land.at[spot], found_land.at[spot], device)
    pass_group.done(unit_land.at[pl.ds(0, rows - 1)])
    got = jnp.where(
        source_row == row, unit_pass[row].astype(F32), unit_land[source_row].astype(F32)
    )
    feat_tail[core, 0] = got[:, :width].astype(BF16)
    feat_tail[core, 1] = got[:, width:].astype(BF16)
    pair_tail = groups.new()
    pair_tail.start(feat_tail.at[core], feat_tail.at[core], partner)
    stat_group.done(stat_land.at[pl.ds(0, plane - 1)])
    stats = stat_land[...]
    tops = stats[:, 0]
    row_top = jnp.max(tops, axis=0, keepdims=True)
    mass = jnp.sum(stats[:, 1] * jnp.exp(tops - row_top), axis=0, keepdims=True)
    log_norm = row_top + jnp.log(mass)
    grads_t = (jnp.exp(scores[...] - log_norm) - hit.astype(F32)).astype(BF16)

    def hold(part, own_base, own_tail):
        rows_here = own_base.shape[0] * base
        own_base[...] = part[:rows_here].reshape(own_base.shape)
        own_tail[...] = part[rows_here:].reshape(own_tail.shape)

    dp_group, dp_tail_group, relay_group, relay_tail_group = [groups.new() for _ in range(4)]

    def send_dp(block, there, mine):
        device = there * plane + spot
        dp_group.start(dp_out_base.at[block], dp_land_base.at[mine], device)
        dp_tail_group.start(dp_out_tail.at[block], dp_land_tail.at[mine], device)

    hold(score_scale * dot(grads_t, all_q[...], 1, 0), dp_own_base, dp_own_tail)
    dp_out_base[...] = dp_own_base[...].astype(BF16)
    dp_out_tail[...] = dp_own_tail[...].astype(BF16)
    if relayed:
        for at, far, near_row, order in (
            (0, 3, 1, (2, 1)), (1, None, None, (2, 0)), (2, None, None, (1, 3)), (3, 0, 2, (1, 2))
        ):

            @pl.when(row == at)
            def _():
                if far is not None:
                    device = near_row * plane + spot
                    relay_group.start(dp_out_base.at[far], dp_relay_base, device)
                    relay_tail_group.start(dp_out_tail.at[far], dp_relay_tail, device)
                for there in order:
                    send_dp(there, there, at)
    else:
        for k in range(1, rows):
            there = lax.rem(row + k, rows)
            send_dp(there, there, row)

    hold(score_scale * dot(grads_t, all_p[...], 0, 0), dq_own_base, dq_own_tail)
    all_lanes = lane_others + [lane]
    pair_groups, pair_tail_group = [groups.new() for _ in all_lanes], groups.new()
    for there, group in zip(all_lanes, pair_groups):
        theirs = 2 * there + 1 - core
        group.start(dq_own_base.at[theirs], dq_pair_base.at[there], partner)
        pair_tail_group.start(dq_own_tail.at[theirs], dq_pair_tail.at[there], partner)
    found_group.done(found_land.at[pl.ds(0, plane - 1)])
    found = jnp.sum(found_land[...][:, 0], axis=0, keepdims=True)
    loss_land[row] = jnp.broadcast_to(
        jnp.sum(log_norm - found, axis=1, keepdims=True), loss_land.shape[1:]
    )
    loss_group = groups.new()
    for device in line_peers:
        loss_group.start(loss_land.at[row], loss_land.at[row], device)
    dq_group, dq_tail_group = groups.new(), groups.new()
    for there, group in zip(all_lanes, pair_groups):
        group.done(dq_pair_base.at[there])
        total = dq_own_base[2 * there + core] + dq_pair_base[there]
        if there is lane:
            dq_mine = total
        else:
            dq_out_base[there] = total.astype(BF16)
            device = row * plane + 2 * there + core
            dq_group.start(dq_out_base.at[there], dq_land_base.at[lane], device)
    pair_tail_group.done(dq_pair_tail.at[pl.ds(0, lanes)])
    for there in lane_others:
        dq_out_tail[there] = (dq_own_tail[2 * there + core] + dq_pair_tail[there]).astype(BF16)
        device = row * plane + 2 * there + core
        dq_tail_group.start(dq_out_tail.at[there], dq_land_tail.at[lane], device)
    dq_mine_tail = dq_own_tail[2 * lane + core] + dq_pair_tail[lane]
    if relayed:
        for at, far in ((1, 3), (2, 0)):

            @pl.when(row == at)
            def _():
                relay_group.landed(dp_relay_base)
                relay_tail_group.landed(dp_relay_tail)
                dp_out_base[far] = (dp_own_base[far] + dp_relay_base[...].astype(F32)).astype(BF16)
                dp_out_tail[far] = (dp_own_tail[far] + dp_relay_tail[...].astype(F32)).astype(BF16)
                send_dp(far, far, at)

    pair_base.done(feat_base.at[0])
    pair_tail.done(feat_tail.at[0])
    x_rows = 4 * base
    all_x[:x_rows] = feat_base[...].reshape(x_rows, width)
    all_x[x_rows:] = flat_rows(feat_tail[...])
    for t in range(TILES):
        start = pl.multiple_of(core * hidden_half + t * tile, 128)
        hidden, slope = gelu_and_slope(dot(all_x[...], w_first[:, pl.ds(start, tile)], 1, 0))
        all_hidden[t] = hidden.T.astype(BF16)
        all_slope[t] = slope
    dq_group.done(dq_land_base.at[pl.ds(0, lanes - 1)])
    dq_tail_group.done(dq_land_tail.at[pl.ds(0, lanes - 1)])
    for there in lane_others:
        dq_mine = dq_mine + dq_land_base[there].astype(F32)
        dq_mine_tail = dq_mine_tail + dq_land_tail[there].astype(F32)
    de_base[core, 0] = dq_mine.astype(BF16)
    de_tail[core, 0] = dq_mine_tail.astype(BF16)

    def send_de(side):
        base_group, tail_group = groups.new(), groups.new()
        base_group.start(de_base.at[core, side], de_base.at[core, side], partner)
        tail_group.start(de_tail.at[core, side], de_tail.at[core, side], partner)

        def finish():
            base_group.done(de_base.at[0, side])
            tail_group.done(de_tail.at[0, side])

        return finish

    finish_pair = [send_de(0)]
    def dp_landed(count):
        dp_group.done(dp_land_base.at[pl.ds(0, count)])
        dp_tail_group.done(dp_land_tail.at[pl.ds(0, count)])

    if relayed:
        ends = lax.rem(row, 3) == 0

        @pl.when(ends)
        def _():
            dp_landed(2)
            relay_group.sent(dp_relay_base)
            relay_tail_group.sent(dp_relay_tail)

        @pl.when(jnp.logical_not(ends))
        def _():
            dp_landed(3)
    else:
        dp_landed(rows - 1)
    dp_mine, dp_mine_tail = dp_own_base[row], dp_own_tail[row]
    for k in range(1, rows):
        there = lax.rem(row + k, rows)
        part, part_tail = dp_land_base[there].astype(F32), dp_land_tail[there].astype(F32)
        if relayed:
            used = jnp.logical_not(jnp.logical_and(ends, row + there == 3))
            part, part_tail = jnp.where(used, part, 0.0), jnp.where(used, part_tail, 0.0)
        dp_mine, dp_mine_tail = dp_mine + part, dp_mine_tail + part_tail
    de_base[core, 1] = dp_mine.astype(BF16)
    de_tail[core, 1] = dp_mine_tail.astype(BF16)
    finish_pair.append(send_de(1))
    low_count, high_count = 2, lanes // 2
    low_lane, high_lane = lax.rem(lane, low_count), lax.div(lane, low_count)
    low_others = [lax.rem(low_lane + k, low_count) for k in range(1, low_count)]
    high_others = [lax.rem(high_lane + k, high_count) for k in range(1, high_count)]
    skip, skip_two = half * lanes, half * high_count

    def in_plane(high, low):
        return plane * row + 2 * (high * low_count + low) + core

    direct = []

    def tile_of(t):
        return t + core * (TILES - 1 - 2 * t)

    def first_stage(chunk_at, part):
        t, cols = chunk_at
        t = tile_of(t)
        for i in range(per_tile):
            for high in range(high_count):
                for low in range(low_count):
                    for j in range(2):
                        at = (((i * high_count + high) * low_count + low) * 2 + j) * chunk
                        piece = part[at : at + chunk]
                        step = t * per_tile + i
                        own[step, j, high, low, :, cols] = piece
                        if j == 0:
                            slot = (low * half + step) * high_count + high
                        else:
                            slot = skip + (high * half + step) * low_count + low
                        outgoing[slot, :, cols] = piece.astype(BF16)
        group = groups.new()
        if chunk_at in direct:
            for away in lane_others:
                high, low = lax.div(away, low_count), lax.rem(away, low_count)
                for i in range(per_tile):
                    step = t * per_tile + i
                    slots = (
                        (low * half + step) * high_count + high,
                        skip + (high * half + step) * low_count + low,
                    )
                    for j in range(2):
                        group.start(
                            outgoing.at[slots[j], :, cols],
                            landing_direct.at[(lane * half + step) * 2 + j],
                            in_plane(high, low),
                        )
            return group
        span = per_tile * high_count
        for low in low_others:
            group.start(
                outgoing.at[pl.ds((low * half + t * per_tile) * high_count, span), :, cols],
                landing.at[pl.ds((low_lane * half + t * per_tile) * high_count, span), :, cols],
                in_plane(high_lane, low),
            )
        span = per_tile * low_count
        for high in high_others:
            group.start(
                outgoing.at[pl.ds(skip + (high * half + t * per_tile) * low_count, span), :, cols],
                landing.at[pl.ds(skip + (high_lane * half + t * per_tile) * low_count, span), :, cols],
                in_plane(high, low_lane),
            )
        return group

    def second_stage(chunk_at, before):
        t, cols = chunk_at
        t = tile_of(t)
        count = (low_count - 1) * high_count + (high_count - 1) * low_count
        before.done(landing.at[pl.ds(0, per_tile * count), :, cols])
        for i in [t * per_tile + n for n in range(per_tile)]:
            for high in range(high_count):
                total = own[i, 0, high, low_lane, :, cols]
                for low in low_others:
                    total = total + landing[(low * half + i) * high_count + high, :, cols].astype(F32)
                own[i, 0, high, low_lane, :, cols] = total
                outgoing_two[high * half + i, :, cols] = total.astype(BF16)
            for low in range(low_count):
                total = own[i, 1, high_lane, low, :, cols]
                for high in high_others:
                    slot = skip + (high * half + i) * low_count + low
                    total = total + landing[slot, :, cols].astype(F32)
                own[i, 1, high_lane, low, :, cols] = total
                outgoing_two[skip_two + low * half + i, :, cols] = total.astype(BF16)
        group = groups.new()
        block = t * per_tile
        for high in high_others:
            group.start(
                outgoing_two.at[pl.ds(high * half + block, per_tile), :, cols],
                landing_two.at[pl.ds(high_lane * half + block, per_tile), :, cols],
                in_plane(high, low_lane),
            )
        for low in low_others:
            group.start(
                outgoing_two.at[pl.ds(skip_two + low * half + block, per_tile), :, cols],
                landing_two.at[pl.ds(skip_two + low_lane * half + block, per_tile), :, cols],
                in_plane(high_lane, low),
            )
        return group

    def line_copy(i, j, cols):
        return pltpu.make_async_remote_copy(
            src_ref=forward.at[i, j, :, cols],
            dst_ref=landed.at[row, :, cols],
            send_sem=line_send.at[i, j],
            recv_sem=line_recv.at[row],
            device_id=(plane * (half * core + i) + column + j,),
            device_id_type=MESH,
        )

    def third_stage(chunk_at, before):
        t, cols = chunk_at
        t = tile_of(t)
        if chunk_at in direct:
            before.done(landing_direct.at[pl.ds(0, (lanes - 1) * per_tile * 2)])
        else:
            count = low_count - 1 + high_count - 1
            before.done(landing_two.at[pl.ds(0, per_tile * count), :, cols])
        for i in [t * per_tile + n for n in range(per_tile)]:
            for j in range(2):
                total = own[i, j, high_lane, low_lane, :, cols]
                if chunk_at in direct:
                    parts = [landing_direct[(away * half + i) * 2 + j] for away in lane_others]
                elif j == 0:
                    parts = [landing_two[high * half + i, :, cols] for high in high_others]
                else:
                    parts = [landing_two[skip_two + low * half + i, :, cols] for low in low_others]
                for landed_part in parts:
                    total = total + landed_part.astype(F32)
                sums[i, j, :, cols] = total
                forward[i, j, :, cols] = total.astype(BF16)

                @pl.when(plane * (half * core + i) + column + j != me)
                def _():
                    line_copy(i, j, cols).start()

    for finish in finish_pair:
        finish()
    de = jnp.concatenate([de_base[...].reshape(x_rows, embed), flat_rows(de_tail[...])], axis=0)
    act_grads = {}

    def part_of(chunk_at):
        t, cols = chunk_at
        if cols.start >= width:
            low = cols.start - width
            return dot(all_hidden[tile_of(t)], de[:, low : low + cols.size], 1, 0)
        if t not in act_grads:
            start = pl.multiple_of(core * hidden_half + tile_of(t) * tile, 128)
            back = dot(de, w_second[pl.ds(start, tile), :], 1, 1)
            act_grads[t] = (all_slope[tile_of(t)] * back).astype(BF16)
        return dot(act_grads[t], all_x[:, cols], 0, 0)

    piece = embed
    chunks = []
    for t in range(TILES):
        chunks.append((t, pl.ds(width, piece)))
        for low in range(0, width, piece):
            chunks.append((t, pl.ds(low, piece)))
    chunks[-1:] = [(TILES - 1, pl.ds(width - piece, piece - LAST))] if LAST < piece else []
    direct.append((TILES - 1, pl.ds(width - LAST, LAST)))
    ones, twos = [], []
    for at in range(len(chunks) + DELAY):
        if at < len(chunks):
            for ahead in range(len(ones), min(at + AHEAD, len(chunks))):
                ones.append(first_stage(chunks[ahead], part_of(chunks[ahead])))
            if at == len(chunks) - 1 - BEHIND:
                last = first_stage(direct[0], part_of(direct[0]))
            twos.append(second_stage(chunks[at], ones[at]))
        if at >= DELAY:
            third_stage(chunks[at - DELAY], twos[at - DELAY])
    third_stage(direct[0], last)

    if relayed:
        for at in range(rows):

            @pl.when(row == at)
            def _():
                p_groups[at].sent(p_base.at[pl.ds(0, 3 if at in (1, 2) else 2)])
                if at in (1, 2):
                    far = 3 if at == 1 else 0
                    p_groups[far].sent(p_base.at[far])

    sender_core = lax.div(row, half)
    whole = pl.ds(0, width + embed)
    for i in range(half):
        for j in range(2):

            @pl.when(plane * (half * core + i) + column + j != me)
            def _():
                line_copy(i, j, whole).wait_send()

    for sender_row in range(rows):
        sender = plane * sender_row + column + sender_core

        @pl.when(sender != me)
        def _():
            pltpu.make_async_remote_copy(
                src_ref=forward.at[0, 0],
                dst_ref=landed.at[sender_row],
                send_sem=line_send.at[0, 0],
                recv_sem=line_recv.at[sender_row],
                device_id=(sender,),
                device_id_type=MESH,
            ).wait_recv()

    total = jnp.where(sender_core == core, sums[lax.rem(row, half), core], 0.0)
    for sender_row in range(rows):
        sender = plane * sender_row + column + sender_core
        total = total + jnp.where(sender == me, 0.0, landed[sender_row].astype(F32))
    out_all[...] = total
    loss_group.done(loss_land.at[pl.ds(0, rows - 1)])
    loss = loss_land[0]
    for k in range(1, rows):
        loss = loss + loss_land[k]
    out_loss[...] = loss * (1.0 / (size * spare))


def split_kernel(loss, total, mean_loss, first, second):
    width = first.shape[1]
    mean_loss[0] = loss[0, 0]
    first[...] = total[:, :width]
    second[...] = total[:, width:]


def split_outputs(loss, total, width):
    vmem = pl.BlockSpec(memory_space=pltpu.VMEM)
    chunk, across = total.shape
    return pl.pallas_call(
        split_kernel,
        out_shape=[
            jax.ShapeDtypeStruct((1,), F32),
            jax.ShapeDtypeStruct((chunk, width), F32),
            jax.ShapeDtypeStruct((chunk, across - width), F32),
        ],
        in_specs=[pl.BlockSpec(memory_space=pltpu.SMEM), vmem],
        out_specs=[pl.BlockSpec(memory_space=pltpu.SMEM), vmem, vmem],
    )(loss, total)


def step(size, plane, score_scale, counts, *arrays):
    query_features, _, positives, w_first, w_second = arrays
    rows, lanes = size // plane, plane // 2
    half = rows // 2
    width, hidden_width = w_first.shape
    embed = w_second.shape[1]
    chunk = hidden_width // size
    across = width + embed
    base = query_features.shape[0] // 2
    unit = base // 16
    block = base + unit
    vmem = pl.BlockSpec(memory_space=pltpu.VMEM)
    anywhere = pl.BlockSpec(memory_space=pl.ANY)
    count = 26 + rows + 2 * lanes + 2 * TILES * (1 + width // embed)

    def split(members, dtype):
        return [
            pltpu.VMEM((members, base, embed), dtype),
            pltpu.VMEM((members, unit, embed), dtype),
        ]

    scratch = [
        pltpu.VMEM((rows, 16 // rows, unit, width), BF16),
        pltpu.VMEM((rows, 16 // rows, unit, width), BF16),
        pltpu.VMEM((16 // rows, rows, unit, width), BF16),
        pltpu.VMEM((16 // rows, rows, unit, width), BF16),
        pltpu.VMEM((rows, unit, 2 * width), BF16),
        pltpu.VMEM((rows, unit, 2 * width), BF16),
        pltpu.VMEM((16,) + positives.shape, F32),
        pltpu.VMEM((2, 2, base, width), BF16),
        pltpu.VMEM((2, 2, unit, width), BF16),
        pltpu.VMEM((plane, base, embed), BF16),
        pltpu.VMEM((rows, base, embed), BF16),
        pltpu.VMEM((plane, unit, embed), BF16),
        pltpu.VMEM((rows, 16 // rows, unit, embed), BF16),
        pltpu.VMEM((16 // rows, rows, unit, embed), BF16),
        pltpu.VMEM((rows, unit, embed), BF16),
        pltpu.VMEM((rows, unit, embed), BF16),
        pltpu.VMEM((rows, rows * unit, embed), BF16),
        pltpu.VMEM((plane, 2, 1, base), F32),
        pltpu.VMEM((plane * block, embed), BF16),
        pltpu.VMEM((rows * block, embed), BF16),
        pltpu.VMEM((rows * block, plane * block), F32),
        pltpu.VMEM((plane, 2, plane * block), F32),
        pltpu.VMEM((plane, 1, plane * block), F32),
        *split(plane, F32),
        *split(lanes, F32),
        *split(lanes, BF16),
        *split(lanes, BF16),
        *split(rows, F32),
        *split(rows, BF16),
        *split(rows, BF16),
        pltpu.VMEM((base, embed), BF16),
        pltpu.VMEM((unit, embed), BF16),
        pltpu.VMEM((rows, 8, 128), F32),
        pltpu.VMEM((2, 2, base, embed), BF16),
        pltpu.VMEM((2, 2, unit, embed), BF16),
        pltpu.VMEM((4 * block, width), BF16),
        pltpu.VMEM((half, 2, lanes // 2, 2, chunk, across), F32),
        pltpu.VMEM((2 * half * lanes, chunk, across), BF16),
        pltpu.VMEM((2 * half * lanes, chunk, across), BF16),
        pltpu.VMEM((half * (lanes // 2 + 2), chunk, across), BF16),
        pltpu.VMEM((half * (lanes // 2 + 2), chunk, across), BF16),
        pltpu.VMEM((2 * half * lanes, chunk, LAST), BF16),
        pltpu.VMEM((half, 2, chunk, across), F32),
        pltpu.VMEM((half, 2, chunk, across), BF16),
        pltpu.VMEM((rows, chunk, across), BF16),
        pltpu.SemaphoreType.DMA((count,)),
        pltpu.SemaphoreType.DMA((count,)),
        pltpu.SemaphoreType.DMA((half, 2)),
        pltpu.SemaphoreType.DMA((rows,)),
        pltpu.VMEM(w_first.shape, BF16),
        pltpu.VMEM(w_second.shape, BF16),
        pltpu.VMEM((TILES, hidden_width // 2 // TILES, 4 * block), BF16),
        pltpu.VMEM((TILES, 4 * block, hidden_width // 2 // TILES), F32),
        pltpu.SemaphoreType.DMA((6,)),
    ]
    return pl.pallas_call(
        functools.partial(step_kernel, size, plane, score_scale),
        out_shape=[
            jax.ShapeDtypeStruct((8, 128), F32),
            jax.ShapeDtypeStruct((chunk, across), F32),
        ],
        in_specs=[pl.BlockSpec(memory_space=pltpu.SMEM)] + [anywhere] * 2 + [vmem]
        + [anywhere] * 2,
        out_specs=[vmem] * 2,
        scratch_shapes=scratch,
        compiler_params=pltpu.CompilerParams(
            collective_id=0, has_side_effects=True, vmem_limit_bytes=60 * 1024 * 1024
        ),
    )(counts, *arrays)


def body(query_features, passage_features, counts, positives, w_first, w_second):
    device_count = lax.axis_size("dp")
    plane = 1 << device_count.bit_length() // 2
    score_scale = 2.5 * w_second.shape[1] ** (-0.5)
    loss, total = step(
        device_count,
        plane,
        score_scale,
        counts,
        query_features,
        passage_features,
        positives[None, :],
        w_first,
        w_second,
    )
    mean_loss, grad_first, grad_second = split_outputs(loss, total, w_first.shape[0])
    return (mean_loss[0], grad_first.T, grad_second)


def solution(mesh):
    return jax.shard_map(
        body,
        mesh=mesh,
        in_specs=(P("dp", None), P("dp", None), P(), P("dp"), P(), P()),
        out_specs=(P(), P(None, "dp"), P("dp", None)),
        check_vma=False,
    )
```

```python
import functools

import jax
import jax.numpy as jnp
from jax import lax
from jax.experimental import pallas as pl
from jax.experimental.pallas import tpu as pltpu
from jax.sharding import PartitionSpec as P

MESH = pl.DeviceIdType.MESH
F32 = jnp.float32
BF16 = jnp.bfloat16
GELU_ROOT = 0.7978845608028654
GELU_CUBE = 0.044715
TILES = 2
AHEAD = 3
DELAY = 2
LAST = 128
BEHIND = 0


def gelu_and_slope(value):
    square = value * value
    bent = jnp.tanh(GELU_ROOT * value * (1.0 + GELU_CUBE * square))
    rise = 0.5 * (1.0 + bent)
    slope = rise + 0.5 * value * (1.0 - bent * bent) * (
        GELU_ROOT * (1.0 + 3.0 * GELU_CUBE * square)
    )
    return value * rise, slope


def dot(left, right, left_dim, right_dim):
    return lax.dot_general(
        left, right, (((left_dim,), (right_dim,)), ((), ())), preferred_element_type=F32
    )


def flat_rows(blocks):
    return blocks.astype(F32).reshape(-1, blocks.shape[-1]).astype(BF16)


class Group:
    def __init__(self, send, recv):
        self.send, self.recv = send, recv

    def start(self, source, landing, device):
        pltpu.make_async_remote_copy(
            src_ref=source,
            dst_ref=landing,
            send_sem=self.send,
            recv_sem=self.recv,
            device_id=(device,),
            device_id_type=MESH,
        ).start()

    def landed(self, span):
        pltpu.make_async_copy(span, span, self.recv).wait()

    def sent(self, span):
        pltpu.make_async_copy(span, span, self.send).wait()

    def done(self, span):
        self.landed(span)
        self.sent(span)


class Groups:
    def __init__(self, send, recv):
        self.send, self.recv, self.used, self.alone = send, recv, 0, 0

    def new_recv(self):
        self.alone += 1
        assert self.used + self.alone <= self.recv.shape[0]
        return self.recv.at[self.recv.shape[0] - self.alone]

    def new(self):
        self.used += 1
        assert self.used <= self.send.shape[0]
        return Group(self.send.at[self.used - 1], self.recv.at[self.used - 1])


def step_kernel(
    size,
    plane,
    score_scale,
    counts,
    query_hbm,
    passage_hbm,
    positives,
    w_first_hbm,
    w_second_hbm,
    out_loss,
    out_all,
    units_q,
    units_p,
    unit_mid_q,
    unit_mid_p,
    unit_pass,
    unit_land,
    unit_pos,
    feat_base,
    feat_tail,
    q_base,
    p_base,
    q_tail,
    q_extra,
    q_mid,
    q_unit,
    q_unit_land,
    p_tails,
    pos_land,
    all_q,
    all_p,
    scores,
    stat_land,
    found_land,
    dq_own_base,
    dq_own_tail,
    dq_pair_base,
    dq_pair_tail,
    dq_out_base,
    dq_out_tail,
    dq_land_base,
    dq_land_tail,
    dp_own_base,
    dp_own_tail,
    dp_out_base,
    dp_out_tail,
    dp_land_base,
    dp_land_tail,
    dp_relay_base,
    dp_relay_tail,
    loss_land,
    de_base,
    de_tail,
    all_x,
    own,
    outgoing,
    landing,
    outgoing_two,
    landing_two,
    landing_direct,
    sums,
    forward,
    landed,
    send_sems,
    recv_sems,
    line_send,
    line_recv,
    w_first,
    w_second,
    all_hidden,
    all_slope,
    load_sems,
):
    me = lax.axis_index("dp")
    rows = size // plane
    half = rows // 2
    lanes = plane // 2
    stride = size // 16
    row = lax.div(me, plane)
    spot = lax.rem(me, plane)
    core = lax.rem(me, 2)
    lane = lax.div(spot, 2)
    column = spot - core
    place = lax.div(me, stride)
    partner = me + 1 - 2 * core
    width, hidden_width = w_first.shape
    embed = w_second.shape[1]
    base = q_base.shape[1]
    unit = unit_pass.shape[1]
    hidden_half = hidden_width // 2
    tile = hidden_half // TILES
    per_tile = half // TILES
    chunk = hidden_half // (half * lanes * 2)
    groups = Groups(send_sems, recv_sems)

    plane_peers = [row * plane + lax.rem(spot + k, plane) for k in range(1, plane)]
    line_peers = [lax.rem(row + k, rows) * plane + spot for k in range(1, rows)]
    bits = [1 << at for at in range(lanes.bit_length() - 1)]
    lane_others = []
    for flips in range(1, lanes):
        away = lane
        for bit in bits:
            if flips & bit:
                away = away + bit - 2 * bit * lax.rem(lax.div(lane, bit), 2)
        lane_others.append(away)
    barrier = pltpu.get_barrier_semaphore()

    def greet(device):
        pl.semaphore_signal(barrier, inc=1, device_id=(device,), device_id_type=MESH)

    for k in range(1, 16):
        greet(lax.rem(place + k, 16) * stride + lax.rem(me, stride))
    for device in plane_peers:
        greet(device)
    in_column = 2 * row + core
    for k in range(1, 2 * rows):
        other = lax.rem(in_column + k, 2 * rows)
        greet(plane * lax.div(other, 2) + column + lax.rem(other, 2))

    spare = base + unit
    near = plane // stride
    aside = lax.div(spot, stride)
    for features, units, sem in ((passage_hbm, units_p, 1), (query_hbm, units_q, 0)):
        for u in range(15):
            there = u + lax.div(u + 16 - place, 16)
            pltpu.make_async_copy(
                features.at[pl.ds(spare + u * unit, unit), :],
                units.at[lax.div(there, near), lax.rem(there, near)],
                load_sems.at[sem],
            ).start()
        pltpu.make_async_copy(
            features.at[pl.ds(base, unit), :], units.at[row, aside], load_sems.at[sem]
        ).start()
    base_loads = [
        pltpu.make_async_copy(
            features.at[pl.ds(0, base), :], feat_base.at[core, at], load_sems.at[2 + at]
        )
        for at, features in enumerate((query_hbm, passage_hbm))
    ]
    weight_loads = [
        pltpu.make_async_copy(w_first_hbm, w_first, load_sems.at[4]),
        pltpu.make_async_copy(w_second_hbm, w_second, load_sems.at[5]),
    ]
    for load in base_loads + weight_loads:
        load.start()
    unit_pos[place] = positives[...].astype(F32)

    pl.semaphore_wait(barrier, 15 + plane - 1 + 2 * rows - 1)

    def units_loaded(features, sem):
        extra = features.at[pl.ds(base, 16 * unit), :]
        pltpu.make_async_copy(extra, extra, load_sems.at[sem]).wait()

    def spread_units(units, unit_mid):
        group = groups.new()
        for k in range(1, near):
            there = lax.rem(aside + k, near)
            group.start(
                units.at[:, there],
                unit_mid.at[aside],
                row * plane + there * stride + lax.rem(me, stride),
            )
        return group

    units_loaded(passage_hbm, 1)
    mid_p_group = spread_units(units_p, unit_mid_p)
    where_group = groups.new()
    for k in range(1, 16):
        device = lax.rem(place + k, 16) * stride + lax.rem(me, stride)
        where_group.start(unit_pos.at[place], unit_pos.at[place], device)

    heavies = []
    for g in range(stride):
        at = jnp.int32(0)
        for k in range(16):
            at = at + jnp.where(counts[g + stride * k] > base, g + stride * k, 0)
        heavies.append(at)
    source = jnp.int32(0)
    for g in range(stride):
        source = source + jnp.where(lax.rem(me, stride) == g, heavies[g], 0)

    def place_of(device):
        found_place = jnp.int32(0)
        for k in range(16):
            found_place = found_place + jnp.where(device >= stride * (k + 1), 1, 0)
        return found_place

    def row_and_aside(at):
        found_row, found_aside = jnp.int32(0), at
        for k in range(1, rows):
            beyond = at >= k * near
            found_row = found_row + jnp.where(beyond, 1, 0)
            found_aside = found_aside - jnp.where(beyond, near, 0)
        return found_row, found_aside

    heavy_place = place_of(source)
    source_row, source_aside = row_and_aside(heavy_place)

    def offset_of(device):
        before = jnp.int32(0)
        for at in heavies:
            before = before + jnp.where(at < device, 1, 0)
        return base * (device + before)

    def tail_row(device):
        piece = lax.div(device, stride) - jnp.where(source < device, 1, 0)
        return jnp.where(source == device, base, spare + unit * piece)

    def tower(features):
        total = None
        for low in range(0, hidden_width, tile):
            act = dot(features, w_first[:, low : low + tile], 1, 0)
            hidden = gelu_and_slope(act)[0].astype(BF16)
            part = dot(hidden, w_second[low : low + tile, :], 1, 0)
            total = part if total is None else total + part
        return total.astype(BF16)

    for load in base_loads:
        load.wait()
    pair_base = groups.new()
    pair_base.start(feat_base.at[core], feat_base.at[core], partner)
    for load in weight_loads:
        load.wait()
    units_loaded(query_hbm, 0)
    extra_x = flat_rows(units_q[...].reshape(16, unit, width))
    first_e = tower(jnp.concatenate([feat_base[core, 1], extra_x], axis=0))
    q_extra[...] = first_e[base:].astype(F32).reshape(q_extra.shape).astype(BF16)
    mid_e_group = spread_units(q_extra, q_mid)
    p_base[row] = first_e[:base]
    p_groups = [groups.new() for _ in range(rows)]
    relayed = rows == 4
    if relayed:

        def p_send(block, there, group):
            group.start(p_base.at[block], p_base.at[block], there * plane + spot)

        for at, order in enumerate(((2, 1), (3, 2, 0), (0, 1, 3), (1, 2))):

            @pl.when(row == at)
            def _():
                for there in order:
                    p_send(at, there, p_groups[at])
    else:
        for k in range(1, rows):
            p_groups[k].start(p_base.at[row], p_base.at[row], line_peers[k - 1])
    q_base[spot] = tower(feat_base[core, 0])
    q_pair = groups.new()
    q_pair.start(q_base.at[spot], q_base.at[spot], partner)
    q_groups = []
    for away in lane_others:
        group = groups.new()
        group.start(q_base.at[spot], q_base.at[spot], row * plane + 2 * away + core)
        q_groups.append(group)
    mid_q_group = spread_units(units_q, unit_mid_q)

    def picked(units, unit_mid):
        return jnp.where(
            source_aside == aside, units[:, aside].astype(F32), unit_mid[source_aside].astype(F32)
        )

    mid_e_group.done(q_mid.at[pl.ds(0, near - 1)])
    q_unit[...] = picked(q_extra, q_mid).astype(BF16)
    q_unit_group = groups.new()
    for k in range(1, rows):
        there = lax.rem(row + k, rows)
        q_unit_group.start(q_unit.at[there], q_unit_land.at[row], there * plane + spot)
    mid_p_group.done(unit_mid_p.at[pl.ds(0, near - 1)])
    passed = picked(units_p, unit_mid_p)
    unit_pass[:, :, width:] = passed.astype(BF16)
    tails = rows * unit
    p_tails[row] = tower(passed.reshape(tails, width).astype(BF16))
    p_tail_group, pass_group = groups.new(), groups.new()
    for device in line_peers:
        p_tail_group.start(p_tails.at[row], p_tails.at[row], device)

    where_group.done(unit_pos.at[pl.ds(0, 15)])
    slots = lax.broadcasted_iota(jnp.int32, (unit, positives.shape[1]), 1)
    chosen = lax.broadcasted_iota(jnp.int32, slots.shape, 0) + tail_row(me)
    tail_pos = jnp.sum(
        jnp.where(slots == chosen, unit_pos[heavy_place], 0.0), axis=1, keepdims=True
    )
    pos_land[spot, 0] = positives[:, :base].astype(F32)
    sub = lax.broadcasted_iota(jnp.int32, (unit, base), 0) + spot * unit
    along = lax.broadcasted_iota(jnp.int32, (unit, base), 1)
    pos_land[spot, 1] = jnp.sum(jnp.where(sub == along, tail_pos, 0.0), axis=0, keepdims=True)
    pos_group = groups.new()
    for device in plane_peers:
        pos_group.start(pos_land.at[spot], pos_land.at[spot], device)

    if relayed:
        for at, (far, end) in ((1, (3, 0)), (2, (0, 3))):

            @pl.when(row == at)
            def _():
                p_groups[far].landed(p_base.at[far])
                p_send(far, end, p_groups[far])

    def forward_q(at):
        there = 2 * lane_others[at] + core
        q_groups[at].done(q_base.at[there])
        q_pair.start(q_base.at[there], q_base.at[there], partner)

    for at in range(lanes - 1):
        forward_q(at)
    q_unit_group.done(q_unit_land.at[pl.ds(0, rows - 1)])
    q_tail[spot] = jnp.where(
        source_row == row, q_unit[row].astype(F32), q_unit_land[source_row].astype(F32)
    ).astype(BF16)
    q_tail_group = groups.new()
    for device in plane_peers:
        q_tail_group.start(q_tail.at[spot], q_tail.at[spot], device)
    if relayed:
        for at in range(rows):
            early = {0: 2, 3: 1}.get(at, at)

            @pl.when(jnp.logical_and(row != at, row != early))
            def _():
                p_groups[at].landed(p_base.at[at])
    else:
        for k in range(1, rows):
            p_groups[k].done(p_base.at[lax.rem(row + rows - k, rows)])
    q_pair.done(q_base.at[pl.ds(0, lanes)])

    q_rows, p_rows = plane * base, rows * base
    line = [plane * k + spot for k in range(rows)]
    base_ids = jnp.concatenate(
        [lax.broadcasted_iota(jnp.int32, (base, 1), 0) + offset_of(device) for device in line],
        axis=0,
    ).astype(F32)
    tail_ids = jnp.concatenate(
        [
            lax.broadcasted_iota(jnp.int32, (unit, 1), 0) + offset_of(source) + tail_row(device)
            for device in line
        ],
        axis=0,
    ).astype(F32)
    all_q[:q_rows] = q_base[...].reshape(q_rows, embed)
    all_p[:p_rows] = p_base[...].reshape(p_rows, embed)
    pos_group.done(pos_land.at[pl.ds(0, plane - 1)])
    base_wanted = jnp.concatenate([pos_land[k, 0] for k in range(plane)], axis=1)

    def spread(value, ids, wanted):
        top = jnp.max(value, axis=0, keepdims=True)
        mass = jnp.sum(jnp.exp(value - top), axis=0, keepdims=True)
        return top, mass, jnp.sum(jnp.where(ids == wanted, value, 0.0), axis=0, keepdims=True)

    def merge(one, two):
        top = jnp.maximum(one[0], two[0])
        mass = one[1] * jnp.exp(one[0] - top) + two[1] * jnp.exp(two[0] - top)
        return top, mass, one[2] + two[2]

    def scored(p_part, q_part):
        scores[p_part, q_part] = score_scale * dot(all_p[p_part], all_q[q_part], 1, 1)
        return scores[p_part, q_part]

    p_base_part, p_tail_part = slice(0, p_rows), slice(p_rows, all_p.shape[0])
    q_base_part, q_tail_part = slice(0, q_rows), slice(q_rows, all_q.shape[0])
    base_stats = spread(scored(p_base_part, q_base_part), base_ids, base_wanted)

    mid_q_group.done(unit_mid_q.at[pl.ds(0, near - 1)])
    unit_pass[:, :, :width] = picked(units_q, unit_mid_q).astype(BF16)
    for k in range(1, rows):
        there = lax.rem(row + k, rows)
        pass_group.start(unit_pass.at[there], unit_land.at[row], there * plane + spot)
    p_tail_group.done(p_tails.at[pl.ds(0, rows - 1)])
    all_p[p_rows:] = p_tails[source_row]
    base_stats = merge(
        base_stats, spread(scored(p_tail_part, q_base_part), tail_ids, base_wanted)
    )
    q_tail_group.done(q_tail.at[pl.ds(0, plane - 1)])
    all_q[q_rows:] = flat_rows(q_tail[...])
    pos_tail = pos_land[0, 1]
    for k in range(1, plane):
        pos_tail = pos_tail + pos_land[k, 1]
    tail_wanted = pos_tail[:, : plane * unit]
    ids = jnp.concatenate([base_ids, tail_ids], axis=0)
    tail_stats = spread(scored(slice(0, all_p.shape[0]), q_tail_part), ids, tail_wanted)
    stat_land[spot, 0:1, :q_rows] = base_stats[0]
    stat_land[spot, 0:1, q_rows:] = tail_stats[0]
    stat_land[spot, 1:2, :q_rows] = base_stats[1]
    stat_land[spot, 1:2, q_rows:] = tail_stats[1]
    found_land[spot, :, :q_rows] = base_stats[2]
    found_land[spot, :, q_rows:] = tail_stats[2]
    wanted = jnp.concatenate([base_wanted, tail_wanted], axis=1)
    hit = ids == wanted
    stat_group, found_group = groups.new(), groups.new()
    for device in plane_peers:
        stat_group.start(stat_land.at[spot], stat_land.at[spot], device)
    for device in plane_peers:
        found_group.start(found_land.at[spot], found_land.at[spot], device)
    pass_group.done(unit_land.at[pl.ds(0, rows - 1)])
    got = jnp.where(
        source_row == row, unit_pass[row].astype(F32), unit_land[source_row].astype(F32)
    )
    feat_tail[core, 0] = got[:, :width].astype(BF16)
    feat_tail[core, 1] = got[:, width:].astype(BF16)
    pair_tail = groups.new()
    pair_tail.start(feat_tail.at[core], feat_tail.at[core], partner)
    stat_group.done(stat_land.at[pl.ds(0, plane - 1)])
    stats = stat_land[...]
    tops = stats[:, 0]
    row_top = jnp.max(tops, axis=0, keepdims=True)
    mass = jnp.sum(stats[:, 1] * jnp.exp(tops - row_top), axis=0, keepdims=True)
    log_norm = row_top + jnp.log(mass)
    grads_t = (jnp.exp(scores[...] - log_norm) - hit.astype(F32)).astype(BF16)

    def hold(part, own_base, own_tail):
        rows_here = own_base.shape[0] * base
        own_base[...] = part[:rows_here].reshape(own_base.shape)
        own_tail[...] = part[rows_here:].reshape(own_tail.shape)

    dp_group, dp_tail_group, relay_group, relay_tail_group = [groups.new() for _ in range(4)]

    def send_dp(block, there, mine):
        device = there * plane + spot
        dp_group.start(dp_out_base.at[block], dp_land_base.at[mine], device)
        dp_tail_group.start(dp_out_tail.at[block], dp_land_tail.at[mine], device)

    hold(score_scale * dot(grads_t, all_q[...], 1, 0), dp_own_base, dp_own_tail)
    dp_out_base[...] = dp_own_base[...].astype(BF16)
    dp_out_tail[...] = dp_own_tail[...].astype(BF16)
    if relayed:
        for at, far, near_row, order in (
            (0, 3, 1, (2, 1)), (1, None, None, (2, 0)), (2, None, None, (1, 3)), (3, 0, 2, (1, 2))
        ):

            @pl.when(row == at)
            def _():
                if far is not None:
                    device = near_row * plane + spot
                    relay_group.start(dp_out_base.at[far], dp_relay_base, device)
                    relay_tail_group.start(dp_out_tail.at[far], dp_relay_tail, device)
                for there in order:
                    send_dp(there, there, at)
    else:
        for k in range(1, rows):
            there = lax.rem(row + k, rows)
            send_dp(there, there, row)

    hold(score_scale * dot(grads_t, all_p[...], 0, 0), dq_own_base, dq_own_tail)
    all_lanes = lane_others + [lane]
    pair_groups, pair_tail_group = [groups.new() for _ in all_lanes], groups.new()
    for there, group in zip(all_lanes, pair_groups):
        theirs = 2 * there + 1 - core
        group.start(dq_own_base.at[theirs], dq_pair_base.at[there], partner)
        pair_tail_group.start(dq_own_tail.at[theirs], dq_pair_tail.at[there], partner)
    found_group.done(found_land.at[pl.ds(0, plane - 1)])
    found = jnp.sum(found_land[...][:, 0], axis=0, keepdims=True)
    loss_land[row] = jnp.broadcast_to(
        jnp.sum(log_norm - found, axis=1, keepdims=True), loss_land.shape[1:]
    )
    loss_group = groups.new()
    for device in line_peers:
        loss_group.start(loss_land.at[row], loss_land.at[row], device)
    dq_group, dq_tail_group = groups.new(), groups.new()
    for there, group in zip(all_lanes, pair_groups):
        group.done(dq_pair_base.at[there])
        total = dq_own_base[2 * there + core] + dq_pair_base[there]
        if there is lane:
            dq_mine = total
        else:
            dq_out_base[there] = total.astype(BF16)
            device = row * plane + 2 * there + core
            dq_group.start(dq_out_base.at[there], dq_land_base.at[lane], device)
    pair_tail_group.done(dq_pair_tail.at[pl.ds(0, lanes)])
    for there in lane_others:
        dq_out_tail[there] = (dq_own_tail[2 * there + core] + dq_pair_tail[there]).astype(BF16)
        device = row * plane + 2 * there + core
        dq_tail_group.start(dq_out_tail.at[there], dq_land_tail.at[lane], device)
    dq_mine_tail = dq_own_tail[2 * lane + core] + dq_pair_tail[lane]
    if relayed:
        for at, far in ((1, 3), (2, 0)):

            @pl.when(row == at)
            def _():
                relay_group.landed(dp_relay_base)
                relay_tail_group.landed(dp_relay_tail)
                dp_out_base[far] = (dp_own_base[far] + dp_relay_base[...].astype(F32)).astype(BF16)
                dp_out_tail[far] = (dp_own_tail[far] + dp_relay_tail[...].astype(F32)).astype(BF16)
                send_dp(far, far, at)

    pair_base.done(feat_base.at[0])
    pair_tail.done(feat_tail.at[0])
    x_rows = 4 * base
    all_x[:x_rows] = feat_base[...].reshape(x_rows, width)
    all_x[x_rows:] = flat_rows(feat_tail[...])
    for t in range(TILES):
        start = pl.multiple_of(core * hidden_half + t * tile, 128)
        hidden, slope = gelu_and_slope(dot(all_x[...], w_first[:, pl.ds(start, tile)], 1, 0))
        all_hidden[t] = hidden.T.astype(BF16)
        all_slope[t] = slope
    dq_group.done(dq_land_base.at[pl.ds(0, lanes - 1)])
    dq_tail_group.done(dq_land_tail.at[pl.ds(0, lanes - 1)])
    for there in lane_others:
        dq_mine = dq_mine + dq_land_base[there].astype(F32)
        dq_mine_tail = dq_mine_tail + dq_land_tail[there].astype(F32)
    de_base[core, 0] = dq_mine.astype(BF16)
    de_tail[core, 0] = dq_mine_tail.astype(BF16)

    def send_de(side):
        base_group, tail_group = groups.new(), groups.new()
        base_group.start(de_base.at[core, side], de_base.at[core, side], partner)
        tail_group.start(de_tail.at[core, side], de_tail.at[core, side], partner)

        def finish():
            base_group.done(de_base.at[0, side])
            tail_group.done(de_tail.at[0, side])

        return finish

    finish_pair = [send_de(0)]
    def dp_landed(count):
        dp_group.done(dp_land_base.at[pl.ds(0, count)])
        dp_tail_group.done(dp_land_tail.at[pl.ds(0, count)])

    if relayed:
        ends = lax.rem(row, 3) == 0

        @pl.when(ends)
        def _():
            dp_landed(2)
            relay_group.sent(dp_relay_base)
            relay_tail_group.sent(dp_relay_tail)

        @pl.when(jnp.logical_not(ends))
        def _():
            dp_landed(3)
    else:
        dp_landed(rows - 1)
    dp_mine, dp_mine_tail = dp_own_base[row], dp_own_tail[row]
    for k in range(1, rows):
        there = lax.rem(row + k, rows)
        part, part_tail = dp_land_base[there].astype(F32), dp_land_tail[there].astype(F32)
        if relayed:
            used = jnp.logical_not(jnp.logical_and(ends, row + there == 3))
            part, part_tail = jnp.where(used, part, 0.0), jnp.where(used, part_tail, 0.0)
        dp_mine, dp_mine_tail = dp_mine + part, dp_mine_tail + part_tail
    de_base[core, 1] = dp_mine.astype(BF16)
    de_tail[core, 1] = dp_mine_tail.astype(BF16)
    finish_pair.append(send_de(1))
    low_count, high_count = 2, lanes // 2
    low_lane, high_lane = lax.rem(lane, low_count), lax.div(lane, low_count)
    low_others = [lax.rem(low_lane + k, low_count) for k in range(1, low_count)]
    high_others = [lax.rem(high_lane + k, high_count) for k in range(1, high_count)]
    skip, skip_two = half * lanes, half * high_count

    def in_plane(high, low):
        return plane * row + 2 * (high * low_count + low) + core

    direct = []
    stage_send = load_sems.at[6]

    def stage_group():
        return Group(stage_send, groups.new_recv())

    def tile_of(t):
        return t + core * (TILES - 1 - 2 * t)

    def first_stage(chunk_at, part):
        t, cols = chunk_at
        t = tile_of(t)
        for i in range(per_tile):
            for high in range(high_count):
                for low in range(low_count):
                    for j in range(2):
                        at = (((i * high_count + high) * low_count + low) * 2 + j) * chunk
                        piece = part[at : at + chunk]
                        step = t * per_tile + i
                        own[step, j, high, low, :, cols] = piece
                        if j == 0:
                            slot = (low * half + step) * high_count + high
                        else:
                            slot = skip + (high * half + step) * low_count + low
                        outgoing[slot, :, cols] = piece.astype(BF16)
        group = stage_group()
        if chunk_at in direct:
            for away in lane_others:
                high, low = lax.div(away, low_count), lax.rem(away, low_count)
                for i in range(per_tile):
                    step = t * per_tile + i
                    slots = (
                        (low * half + step) * high_count + high,
                        skip + (high * half + step) * low_count + low,
                    )
                    for j in range(2):
                        group.start(
                            outgoing.at[slots[j], :, cols],
                            landing_direct.at[(lane * half + step) * 2 + j],
                            in_plane(high, low),
                        )
            return group
        span = per_tile * high_count
        for low in low_others:
            group.start(
                outgoing.at[pl.ds((low * half + t * per_tile) * high_count, span), :, cols],
                landing.at[pl.ds((low_lane * half + t * per_tile) * high_count, span), :, cols],
                in_plane(high_lane, low),
            )
        span = per_tile * low_count
        for high in high_others:
            group.start(
                outgoing.at[pl.ds(skip + (high * half + t * per_tile) * low_count, span), :, cols],
                landing.at[pl.ds(skip + (high_lane * half + t * per_tile) * low_count, span), :, cols],
                in_plane(high, low_lane),
            )
        return group

    def second_stage(chunk_at, before):
        t, cols = chunk_at
        t = tile_of(t)
        count = (low_count - 1) * high_count + (high_count - 1) * low_count
        before.landed(landing.at[pl.ds(0, per_tile * count), :, cols])
        for i in [t * per_tile + n for n in range(per_tile)]:
            for high in range(high_count):
                total = own[i, 0, high, low_lane, :, cols]
                for low in low_others:
                    total = total + landing[(low * half + i) * high_count + high, :, cols].astype(F32)
                own[i, 0, high, low_lane, :, cols] = total
                outgoing_two[high * half + i, :, cols] = total.astype(BF16)
            for low in range(low_count):
                total = own[i, 1, high_lane, low, :, cols]
                for high in high_others:
                    slot = skip + (high * half + i) * low_count + low
                    total = total + landing[slot, :, cols].astype(F32)
                own[i, 1, high_lane, low, :, cols] = total
                outgoing_two[skip_two + low * half + i, :, cols] = total.astype(BF16)
        group = stage_group()
        block = t * per_tile
        for high in high_others:
            group.start(
                outgoing_two.at[pl.ds(high * half + block, per_tile), :, cols],
                landing_two.at[pl.ds(high_lane * half + block, per_tile), :, cols],
                in_plane(high, low_lane),
            )
        for low in low_others:
            group.start(
                outgoing_two.at[pl.ds(skip_two + low * half + block, per_tile), :, cols],
                landing_two.at[pl.ds(skip_two + low_lane * half + block, per_tile), :, cols],
                in_plane(high_lane, low),
            )
        return group

    def line_copy(i, j, cols):
        return pltpu.make_async_remote_copy(
            src_ref=forward.at[i, j, :, cols],
            dst_ref=landed.at[row, :, cols],
            send_sem=line_send.at[i, j],
            recv_sem=line_recv.at[row],
            device_id=(plane * (half * core + i) + column + j,),
            device_id_type=MESH,
        )

    def third_stage(chunk_at, before):
        t, cols = chunk_at
        t = tile_of(t)
        if chunk_at in direct:
            before.landed(landing_direct.at[pl.ds(0, (lanes - 1) * per_tile * 2)])
        else:
            count = low_count - 1 + high_count - 1
            before.landed(landing_two.at[pl.ds(0, per_tile * count), :, cols])
        for i in [t * per_tile + n for n in range(per_tile)]:
            for j in range(2):
                total = own[i, j, high_lane, low_lane, :, cols]
                if chunk_at in direct:
                    parts = [landing_direct[(away * half + i) * 2 + j] for away in lane_others]
                elif j == 0:
                    parts = [landing_two[high * half + i, :, cols] for high in high_others]
                else:
                    parts = [landing_two[skip_two + low * half + i, :, cols] for low in low_others]
                for landed_part in parts:
                    total = total + landed_part.astype(F32)
                sums[i, j, :, cols] = total
                forward[i, j, :, cols] = total.astype(BF16)

                @pl.when(plane * (half * core + i) + column + j != me)
                def _():
                    line_copy(i, j, cols).start()

    for finish in finish_pair:
        finish()
    de = jnp.concatenate([de_base[...].reshape(x_rows, embed), flat_rows(de_tail[...])], axis=0)
    act_grads = {}

    def part_of(chunk_at):
        t, cols = chunk_at
        if cols.start >= width:
            low = cols.start - width
            return dot(all_hidden[tile_of(t)], de[:, low : low + cols.size], 1, 0)
        if t not in act_grads:
            start = pl.multiple_of(core * hidden_half + tile_of(t) * tile, 128)
            back = dot(de, w_second[pl.ds(start, tile), :], 1, 1)
            act_grads[t] = (all_slope[tile_of(t)] * back).astype(BF16)
        return dot(act_grads[t], all_x[:, cols], 0, 0)

    piece = embed
    chunks = []
    for t in range(TILES):
        chunks.append((t, pl.ds(width, piece)))
        for low in range(0, width, piece):
            chunks.append((t, pl.ds(low, piece)))
    chunks[-1:] = [(TILES - 1, pl.ds(width - piece, piece - LAST))] if LAST < piece else []
    direct.append((TILES - 1, pl.ds(width - LAST, LAST)))
    ones, twos = [], []
    for at in range(len(chunks) + DELAY):
        if at < len(chunks):
            for ahead in range(len(ones), min(at + AHEAD, len(chunks))):
                ones.append(first_stage(chunks[ahead], part_of(chunks[ahead])))
            if at == len(chunks) - 1 - BEHIND:
                last = first_stage(direct[0], part_of(direct[0]))
            twos.append(second_stage(chunks[at], ones[at]))
        if at >= DELAY:
            third_stage(chunks[at - DELAY], twos[at - DELAY])
    third_stage(direct[0], last)
    all_sent = landing.at[pl.ds(0, 2 * half * (lanes - 1))]
    pltpu.make_async_copy(all_sent, all_sent, stage_send).wait()

    if relayed:
        for at in range(rows):

            @pl.when(row == at)
            def _():
                p_groups[at].sent(p_base.at[pl.ds(0, 3 if at in (1, 2) else 2)])
                if at in (1, 2):
                    far = 3 if at == 1 else 0
                    p_groups[far].sent(p_base.at[far])

    sender_core = lax.div(row, half)
    whole = pl.ds(0, width + embed)
    for i in range(half):
        for j in range(2):

            @pl.when(plane * (half * core + i) + column + j != me)
            def _():
                line_copy(i, j, whole).wait_send()

    for sender_row in range(rows):
        sender = plane * sender_row + column + sender_core

        @pl.when(sender != me)
        def _():
            pltpu.make_async_remote_copy(
                src_ref=forward.at[0, 0],
                dst_ref=landed.at[sender_row],
                send_sem=line_send.at[0, 0],
                recv_sem=line_recv.at[sender_row],
                device_id=(sender,),
                device_id_type=MESH,
            ).wait_recv()

    total = jnp.where(sender_core == core, sums[lax.rem(row, half), core], 0.0)
    for sender_row in range(rows):
        sender = plane * sender_row + column + sender_core
        total = total + jnp.where(sender == me, 0.0, landed[sender_row].astype(F32))
    out_all[...] = total
    loss_group.done(loss_land.at[pl.ds(0, rows - 1)])
    loss = loss_land[0]
    for k in range(1, rows):
        loss = loss + loss_land[k]
    out_loss[...] = loss * (1.0 / (size * spare))


def split_kernel(loss, total, mean_loss, first, second):
    width = first.shape[1]
    mean_loss[0] = loss[0, 0]
    first[...] = total[:, :width]
    second[...] = total[:, width:]


def split_outputs(loss, total, width):
    vmem = pl.BlockSpec(memory_space=pltpu.VMEM)
    chunk, across = total.shape
    return pl.pallas_call(
        split_kernel,
        out_shape=[
            jax.ShapeDtypeStruct((1,), F32),
            jax.ShapeDtypeStruct((chunk, width), F32),
            jax.ShapeDtypeStruct((chunk, across - width), F32),
        ],
        in_specs=[pl.BlockSpec(memory_space=pltpu.SMEM), vmem],
        out_specs=[pl.BlockSpec(memory_space=pltpu.SMEM), vmem, vmem],
    )(loss, total)


def step(size, plane, score_scale, counts, *arrays):
    query_features, _, positives, w_first, w_second = arrays
    rows, lanes = size // plane, plane // 2
    half = rows // 2
    width, hidden_width = w_first.shape
    embed = w_second.shape[1]
    chunk = hidden_width // size
    across = width + embed
    base = query_features.shape[0] // 2
    unit = base // 16
    block = base + unit
    vmem = pl.BlockSpec(memory_space=pltpu.VMEM)
    anywhere = pl.BlockSpec(memory_space=pl.ANY)
    count = 25 + rows + 2 * lanes
    alone = 2 * TILES * (1 + width // embed) + 1

    def split(members, dtype):
        return [
            pltpu.VMEM((members, base, embed), dtype),
            pltpu.VMEM((members, unit, embed), dtype),
        ]

    scratch = [
        pltpu.VMEM((rows, 16 // rows, unit, width), BF16),
        pltpu.VMEM((rows, 16 // rows, unit, width), BF16),
        pltpu.VMEM((16 // rows, rows, unit, width), BF16),
        pltpu.VMEM((16 // rows, rows, unit, width), BF16),
        pltpu.VMEM((rows, unit, 2 * width), BF16),
        pltpu.VMEM((rows, unit, 2 * width), BF16),
        pltpu.VMEM((16,) + positives.shape, F32),
        pltpu.VMEM((2, 2, base, width), BF16),
        pltpu.VMEM((2, 2, unit, width), BF16),
        pltpu.VMEM((plane, base, embed), BF16),
        pltpu.VMEM((rows, base, embed), BF16),
        pltpu.VMEM((plane, unit, embed), BF16),
        pltpu.VMEM((rows, 16 // rows, unit, embed), BF16),
        pltpu.VMEM((16 // rows, rows, unit, embed), BF16),
        pltpu.VMEM((rows, unit, embed), BF16),
        pltpu.VMEM((rows, unit, embed), BF16),
        pltpu.VMEM((rows, rows * unit, embed), BF16),
        pltpu.VMEM((plane, 2, 1, base), F32),
        pltpu.VMEM((plane * block, embed), BF16),
        pltpu.VMEM((rows * block, embed), BF16),
        pltpu.VMEM((rows * block, plane * block), F32),
        pltpu.VMEM((plane, 2, plane * block), F32),
        pltpu.VMEM((plane, 1, plane * block), F32),
        *split(plane, F32),
        *split(lanes, F32),
        *split(lanes, BF16),
        *split(lanes, BF16),
        *split(rows, F32),
        *split(rows, BF16),
        *split(rows, BF16),
        pltpu.VMEM((base, embed), BF16),
        pltpu.VMEM((unit, embed), BF16),
        pltpu.VMEM((rows, 8, 128), F32),
        pltpu.VMEM((2, 2, base, embed), BF16),
        pltpu.VMEM((2, 2, unit, embed), BF16),
        pltpu.VMEM((4 * block, width), BF16),
        pltpu.VMEM((half, 2, lanes // 2, 2, chunk, across), F32),
        pltpu.VMEM((2 * half * lanes, chunk, across), BF16),
        pltpu.VMEM((2 * half * lanes, chunk, across), BF16),
        pltpu.VMEM((half * (lanes // 2 + 2), chunk, across), BF16),
        pltpu.VMEM((half * (lanes // 2 + 2), chunk, across), BF16),
        pltpu.VMEM((2 * half * lanes, chunk, LAST), BF16),
        pltpu.VMEM((half, 2, chunk, across), F32),
        pltpu.VMEM((half, 2, chunk, across), BF16),
        pltpu.VMEM((rows, chunk, across), BF16),
        pltpu.SemaphoreType.DMA((count,)),
        pltpu.SemaphoreType.DMA((count + alone,)),
        pltpu.SemaphoreType.DMA((half, 2)),
        pltpu.SemaphoreType.DMA((rows,)),
        pltpu.VMEM(w_first.shape, BF16),
        pltpu.VMEM(w_second.shape, BF16),
        pltpu.VMEM((TILES, hidden_width // 2 // TILES, 4 * block), BF16),
        pltpu.VMEM((TILES, 4 * block, hidden_width // 2 // TILES), F32),
        pltpu.SemaphoreType.DMA((7,)),
    ]
    return pl.pallas_call(
        functools.partial(step_kernel, size, plane, score_scale),
        out_shape=[
            jax.ShapeDtypeStruct((8, 128), F32),
            jax.ShapeDtypeStruct((chunk, across), F32),
        ],
        in_specs=[pl.BlockSpec(memory_space=pltpu.SMEM)] + [anywhere] * 2 + [vmem]
        + [anywhere] * 2,
        out_specs=[vmem] * 2,
        scratch_shapes=scratch,
        compiler_params=pltpu.CompilerParams(
            collective_id=0, has_side_effects=True, vmem_limit_bytes=60 * 1024 * 1024
        ),
    )(counts, *arrays)


def body(query_features, passage_features, counts, positives, w_first, w_second):
    device_count = lax.axis_size("dp")
    plane = 1 << device_count.bit_length() // 2
    score_scale = 2.5 * w_second.shape[1] ** (-0.5)
    loss, total = step(
        device_count,
        plane,
        score_scale,
        counts,
        query_features,
        passage_features,
        positives[None, :],
        w_first,
        w_second,
    )
    mean_loss, grad_first, grad_second = split_outputs(loss, total, w_first.shape[0])
    return (mean_loss[0], grad_first.T, grad_second)


def solution(mesh):
    return jax.shard_map(
        body,
        mesh=mesh,
        in_specs=(P("dp", None), P("dp", None), P(), P("dp"), P(), P()),
        out_specs=(P(), P(None, "dp"), P("dp", None)),
        check_vma=False,
    )
```
